128 devices in a mesh: seq: 32 (over z, x, core), mp: 4 (over y).
Axes of the slice: x: 4, y: 4, z: 4, core: 2. Of those that a mesh axis runs over, the one named last changes fastest.
Arguments:
- teacher_query: bfloat16 [5120, 8192], P('seq', 'mp'), may hold values from -37 to 37
- teacher_keys: bfloat16 [5120, 1024], P('seq', 'mp'), may hold values from -4 to 4
- teacher_values: bfloat16 [5120, 1024], P('seq', 'mp'), may hold values from -4 to 4
- teacher_docs: int32 [16], replicated, may hold values from 1 to 3840, 5120 in all
- student_query: bfloat16 [5120, 3584], P('seq', 'mp'), may hold values from -37 to 37
- student_keys: bfloat16 [5120, 512], P('seq', 'mp'), may hold values from -4 to 4
- student_values: bfloat16 [5120, 512], P('seq', 'mp'), may hold values from -4 to 4
- student_docs: int32 [16], replicated, may hold values from 1 to 3840, 5120 in all
- projector: bfloat16 [8192, 3584], P('mp'), may hold values from -0.125 to 0.125
- teacher_spans: int32 [32, 2, 128], P('seq'), may hold values from 0 to 159, as said below
- student_spans: int32 [32, 2, 128], P('seq'), may hold values from 0 to 159, as said below
Outputs:
- grad_query: bfloat16 [5120, 3584], P('seq', 'mp')
- grad_keys: bfloat16 [5120, 512], P('seq', 'mp')
- grad_values: bfloat16 [5120, 512], P('seq', 'mp')
The draws below stay inside these ranges and needn't reach their ends.
Inputs may be any that keep to these rules, and one draw needn't show every extreme that they name: `teacher_spans`: column d * 4 + c of row r holds, first, the first teacher position of a span (counted within the 160 positions of index r along seq) and, second, its number of positions; it is the c-th span that index r sends to index d. A count of 0 marks an empty slot; the live slots of one destination come first; live spans cover 1 to 4 positions inside the index's positions and may intersect. One source sends at most 4 spans to one destination, and in every draw some destination receives 4 from every source. `student_spans`: column r * 4 + c of row d holds the student range (first position within the 160 positions of index d along seq, then the number of positions) of the span in column d * 4 + c of row r of teacher_spans; the count is 0 exactly where that teacher slot is empty, else 1 to 4. Ranges may intersect.
All inputs are finite; a program needn't handle non-finite values.
Results may differ from the reference program's by a relative error of at most 0.015.
Values may be sent and summed in bfloat16 or wider, within the bound.
A program may use at most 128 MiB of HBM per device.

```python
import math
import jax
import jax.numpy as jnp
import numpy as np
from jax import lax

DT = 8192
HT = 64
KVT = 8
HD = 128
DS = 3584
HS = 28
KVS = 4
TOK_DEV = 160
NDOCS = 16
CAP = 4
SPAN_MAX = 4
TOKENS = 5120
N_SEQ = 32


def drawn_keys(key, groups, salt_value):
    base_key = jax.random.fold_in(key, salt_value)
    entries_keys = jnp.clip(jax.random.normal(base_key, (TOKENS, groups * HD), jnp.float32), -4.0, 4.0)
    keys_out = entries_keys
    return keys_out


def drawn_queries(key, heads, salt_value):
    base_key = jax.random.fold_in(key, salt_value + 3)
    return jnp.clip(3.0 * jax.random.normal(base_key, (TOKENS, heads * HD), jnp.float32), -12.0, 12.0)


def draw_teacher_query(key, part):
    return drawn_queries(key, HT, 11).astype(jnp.bfloat16)


def draw_teacher_keys(key, part):
    return drawn_keys(key, KVT, 11).astype(jnp.bfloat16)


def draw_student_query(key, part):
    return drawn_queries(key, HS, 31).astype(jnp.bfloat16)


def draw_student_keys(key, part):
    return drawn_keys(key, KVS, 31).astype(jnp.bfloat16)


def span_tables(key):
    rank_count = TOKENS // TOK_DEV
    slot_count = rank_count * CAP
    busy_dest = jax.random.randint(jax.random.fold_in(key, 701), (rank_count,), 0, 4) == 0
    forced = jax.random.randint(jax.random.fold_in(key, 702), (), 0, rank_count)
    heavy_counts = jax.random.randint(jax.random.fold_in(key, 703), (rank_count, rank_count), 0, CAP + 1)
    light_counts = jax.random.randint(jax.random.fold_in(key, 704), (rank_count, rank_count), 1, CAP)
    send_counts = jnp.where(busy_dest[None, :], heavy_counts, light_counts)
    send_counts = jnp.where(jnp.arange(rank_count, dtype=jnp.int32)[None, :] == forced, CAP, send_counts)
    live_slots = jnp.arange(CAP, dtype=jnp.int32)[None, None, :] < send_counts[:, :, None]
    send_live = live_slots.reshape(rank_count, slot_count)
    recv_live = jnp.transpose(live_slots, (1, 0, 2)).reshape(rank_count, slot_count)
    teacher_len = jnp.where(send_live, jax.random.randint(jax.random.fold_in(key, 705), (rank_count, slot_count), 1, SPAN_MAX + 1), 0)
    teacher_first = jnp.where(send_live, jax.random.randint(jax.random.fold_in(key, 706), (rank_count, slot_count), 0, TOK_DEV - teacher_len + 1), 0)
    student_len = jnp.where(recv_live, jax.random.randint(jax.random.fold_in(key, 707), (rank_count, slot_count), 1, SPAN_MAX + 1), 0)
    student_first = jnp.where(recv_live, jax.random.randint(jax.random.fold_in(key, 708), (rank_count, slot_count), 0, TOK_DEV - student_len + 1), 0)
    teacher_table = jnp.stack([teacher_first, teacher_len], axis=1).astype(jnp.int32)
    student_table = jnp.stack([student_first, student_len], axis=1).astype(jnp.int32)
    return (teacher_table, student_table)


def draw_teacher_spans(key, part):
    return span_tables(key)[0]


def draw_student_spans(key, part):
    return span_tables(key)[1]


def block_levels(rng, extent, pieces, least, high):
    loudness, own = 1.0, jax.random.fold_in(rng, 6)
    for dim, blocks in pieces:
        heights = jnp.exp(jax.random.uniform(jax.random.fold_in(own, dim), (blocks,), jnp.float32, least / len(pieces), high / len(pieces)))
        loudness = loudness * jnp.repeat(heights, extent[dim] // blocks).reshape([-1 if axis == dim else 1 for axis in range(len(extent))])
    return loudness


def split_up(number_of, total, reach, skew):
    loads = [(1 << 20) // math.isqrt(standing ** skew) + 1 for standing in range(2, number_of + 1)]
    spare, holding = total - reach - (number_of - 1), [1] * (number_of - 1)
    while spare > 0:
        candidates = [i for i in range(number_of - 1) if holding[i] < reach]
        whole, budget = sum([loads[i] for i in candidates]), spare
        for i in candidates:
            addition = min(reach - holding[i], max(1, budget * loads[i] // whole), spare)
            holding[i] = holding[i] + addition
            spare = spare - addition
    return np.array([reach] + holding)


def ragged(own_key, count, total, most, skew):
    if count == 2:
        one = jax.random.randint(own_key, (), max(1, total - most), min(most, total - 1) + 1)
        return jnp.stack([one, total - one])
    sizes = jnp.asarray(split_up(count, total, most, skew), jnp.int32)
    couples = (count - 1) // 2
    donor, receiver = sizes[1:1 + 2 * couples:2], sizes[2:2 + 2 * couples:2]
    room = jnp.minimum(donor - 1, most - receiver)
    shifted = jax.random.randint(jax.random.fold_in(own_key, 1), (couples,), 0, 1 << 20) % (room + 1)
    sizes = sizes.at[1:1 + 2 * couples:2].set(donor - shifted).at[2:2 + 2 * couples:2].set(receiver + shifted)
    return sizes[jax.random.permutation(jax.random.fold_in(own_key, 2), count)]


def noise(key, dims, scale, reach, split=(), held_as=jnp.bfloat16):
    gain = block_levels(key, dims, split, -0.22, 0.18) if split else 1.0
    result = jax.random.normal(key, dims, jnp.float32) * scale * gain
    return jnp.minimum(jnp.maximum(result, -reach), reach).astype(held_as)


def setup_inputs(seed: int = 0) -> dict:
    key_list = jax.random.split(jax.random.key(seed), 12)
    teacher_query = draw_teacher_query(jax.random.fold_in(key_list[11], 71), 0)
    teacher_keys = draw_teacher_keys(jax.random.fold_in(key_list[11], 71), 0)
    teacher_values = noise(key_list[2], (TOKENS, KVT * HD), 1.0, 4.0, ((0, 32), (1, 4)))
    teacher_docs = ragged(key_list[3], NDOCS, TOKENS, 3 * TOKENS // 4, 2).astype(jnp.int32)
    student_query = draw_student_query(jax.random.fold_in(key_list[11], 71), 0)
    student_keys = draw_student_keys(jax.random.fold_in(key_list[11], 71), 0)
    student_values = noise(key_list[6], (TOKENS, KVS * HD), 1.0, 4.0, ((0, 32), (1, 4)))
    student_docs = ragged(key_list[7], NDOCS, TOKENS, 3 * TOKENS // 4, 2).astype(jnp.int32)
    projector = noise(key_list[8], (DT, DS), (DT // 4) ** -0.5, 0.125, ((0, 4),))
    teacher_spans = draw_teacher_spans(jax.random.fold_in(key_list[11], 71), 0)
    student_spans = draw_student_spans(jax.random.fold_in(key_list[11], 71), 0)
    return {"teacher_query": teacher_query, "teacher_keys": teacher_keys, "teacher_values": teacher_values, "teacher_docs": teacher_docs, "student_query": student_query, "student_keys": student_keys, "student_values": student_values, "student_docs": student_docs, "projector": projector, "teacher_spans": teacher_spans, "student_spans": student_spans}


NEG = -1e30


def doc_index(lengths, positions):
    bounds = jnp.cumsum(lengths)
    return jnp.sum((bounds[None, :] <= positions[:, None]).astype(jnp.int32), axis=1)


def block_size(total_rows):
    size_now = min(512, total_rows)
    while total_rows % size_now:
        size_now -= 1
    return size_now


def to_bfloat(values_in):
    lowered = values_in.astype(jnp.bfloat16)
    lowered = lax.optimization_barrier(lowered)
    return lowered.astype(jnp.float32)


def members(starts, lengths, tok_rows):
    places = jnp.arange(tok_rows, dtype=jnp.int32)
    inside = (places[None, :] >= starts[:, None]) & (places[None, :] < (starts + lengths)[:, None])
    return inside.astype(jnp.float32), 1.0 / jnp.maximum(lengths, 1).astype(jnp.float32)


def forward(query_in, key_in, value_in, docs, heads, groups):
    total_rows = query_in.shape[0]
    head_ratio = heads // groups
    score_scale = HD ** -0.5
    positions = jnp.arange(total_rows, dtype=jnp.int32)
    doc_ids = doc_index(docs, positions)
    step_rows = block_size(total_rows)
    count_blocks = total_rows // step_rows
    query_blocks = query_in.astype(jnp.float32).reshape(count_blocks, step_rows, groups, head_ratio, HD)
    key_wide = jnp.moveaxis(key_in.astype(jnp.float32).reshape(total_rows, groups, HD), 1, 0)
    value_wide = jnp.moveaxis(value_in.astype(jnp.float32).reshape(total_rows, groups, HD), 1, 0)

    def one_block(inputs):
        number, query_block = inputs
        rows_here = number * step_rows + jnp.arange(step_rows, dtype=jnp.int32)
        allowed = (doc_ids[None, :] == doc_index(docs, rows_here)[:, None]) & (positions[None, :] <= rows_here[:, None])

        def one_group(group_inputs):
            query_group, key_group, value_group = group_inputs
            scores = jnp.einsum("qrd,kd->rqk", query_group, key_group, precision=lax.Precision.HIGHEST) * score_scale
            scores = jnp.where(allowed[None], scores, NEG)
            row_peak = jnp.max(scores, axis=-1)
            weights = jnp.where(allowed[None], jnp.exp(scores - row_peak[..., None]), 0.0)
            totals = jnp.sum(weights, axis=-1)
            contrib = jnp.einsum("rqk,kd->rqd", to_bfloat(weights), value_group, precision=lax.Precision.HIGHEST)
            return contrib / totals[..., None], row_peak + jnp.log(totals)

        contexts, log_sums = lax.map(one_group, (jnp.moveaxis(query_block, 1, 0), key_wide, value_wide))
        contexts = jnp.transpose(contexts, (2, 0, 1, 3)).reshape(step_rows, heads * HD)
        log_sums = jnp.transpose(log_sums, (2, 0, 1)).reshape(step_rows, heads)
        return contexts, log_sums

    contexts, log_sums = lax.map(one_block, (jnp.arange(count_blocks, dtype=jnp.int32), query_blocks))
    return contexts.reshape(total_rows, heads * HD).astype(jnp.bfloat16), log_sums.reshape(total_rows, heads)


def backward(query_in, key_in, value_in, docs, heads, groups, context, log_sums, grad_out):
    total_rows = query_in.shape[0]
    head_ratio = heads // groups
    score_scale = HD ** -0.5
    positions = jnp.arange(total_rows, dtype=jnp.int32)
    doc_ids = doc_index(docs, positions)
    step_rows = block_size(total_rows)
    count_blocks = total_rows // step_rows
    deltas = jnp.sum((grad_out.astype(jnp.float32) * context.astype(jnp.float32)).reshape(total_rows, heads, HD), axis=-1)
    queries = query_in.astype(jnp.float32).reshape(count_blocks, step_rows, groups, head_ratio, HD)
    douts = grad_out.astype(jnp.float32).reshape(count_blocks, step_rows, groups, head_ratio, HD)
    sum_blocks = log_sums.reshape(count_blocks, step_rows, groups, head_ratio)
    delta_blocks = deltas.reshape(count_blocks, step_rows, groups, head_ratio)
    key_wide = jnp.moveaxis(key_in.astype(jnp.float32).reshape(total_rows, groups, HD), 1, 0)
    value_wide = jnp.moveaxis(value_in.astype(jnp.float32).reshape(total_rows, groups, HD), 1, 0)

    def one_block(carried, inputs):
        number, query_block, dout_block, sum_block, delta_block = inputs
        rows_here = number * step_rows + jnp.arange(step_rows, dtype=jnp.int32)
        allowed = (doc_ids[None, :] == doc_index(docs, rows_here)[:, None]) & (positions[None, :] <= rows_here[:, None])

        def one_group(group_inputs):
            query_group, dout_group, sum_group, delta_group, key_group, value_group = group_inputs
            scores = jnp.einsum("qrd,kd->rqk", query_group, key_group, precision=lax.Precision.HIGHEST) * score_scale
            probs = jnp.where(allowed[None], jnp.exp(scores - jnp.transpose(sum_group)[:, :, None]), 0.0)
            prob_grad = jnp.einsum("qrd,kd->rqk", dout_group, value_group, precision=lax.Precision.HIGHEST)
            dscore = to_bfloat(probs * (prob_grad - jnp.transpose(delta_group)[:, :, None]))
            probs_low = to_bfloat(probs)
            query_grad = jnp.einsum("rqk,kd->qrd", dscore, key_group, precision=lax.Precision.HIGHEST) * score_scale
            key_grad = jnp.einsum("rqk,qrd->kd", dscore, query_group, precision=lax.Precision.HIGHEST) * score_scale
            value_grad = jnp.einsum("rqk,qrd->kd", probs_low, dout_group, precision=lax.Precision.HIGHEST)
            return query_grad, key_grad, value_grad

        query_grad, key_grad, value_grad = lax.map(one_group, (jnp.moveaxis(query_block, 1, 0), jnp.moveaxis(dout_block, 1, 0), jnp.moveaxis(sum_block, 1, 0), jnp.moveaxis(delta_block, 1, 0), key_wide, value_wide))
        query_grad = jnp.moveaxis(query_grad, 0, 1).reshape(step_rows, heads * HD)
        return (carried[0] + key_grad, carried[1] + value_grad), query_grad

    start_sums = (jnp.zeros((groups, total_rows, HD), jnp.float32), jnp.zeros((groups, total_rows, HD), jnp.float32))
    sums_out, query_grads = lax.scan(one_block, start_sums, (jnp.arange(count_blocks, dtype=jnp.int32), queries, douts, sum_blocks, delta_blocks))
    grad_keys = jnp.moveaxis(sums_out[0], 0, 1).reshape(total_rows, groups * HD).astype(jnp.bfloat16)
    grad_values = jnp.moveaxis(sums_out[1], 0, 1).reshape(total_rows, groups * HD).astype(jnp.bfloat16)
    return query_grads.reshape(total_rows, heads * HD).astype(jnp.bfloat16), grad_keys, grad_values


def reference(teacher_query, teacher_keys, teacher_values, teacher_docs, student_query, student_keys, student_values, student_docs, projector, teacher_spans, student_spans):
    teacher_context, unused = forward(teacher_query, teacher_keys, teacher_values, teacher_docs, HT, KVT)
    student_context, student_sums = forward(student_query, student_keys, student_values, student_docs, HS, KVS)
    rank_count = N_SEQ
    projector_wide = projector.astype(jnp.float32)

    def teacher_rank(inputs):
        spans, context = inputs
        inside, weights = members(spans[0], spans[1], TOK_DEV)
        pooled = jnp.dot(inside, context.astype(jnp.float32), precision=lax.Precision.HIGHEST) * weights[:, None]
        pooled = to_bfloat(pooled)
        return jnp.dot(pooled, projector_wide, precision=lax.Precision.HIGHEST).astype(jnp.bfloat16)

    targets = lax.map(teacher_rank, (teacher_spans, teacher_context.reshape(rank_count, TOK_DEV, DT)))
    arrived = jnp.transpose(targets.reshape(rank_count, rank_count, CAP, DS), (1, 0, 2, 3)).reshape(rank_count, rank_count * CAP, DS)

    def student_rank(inputs):
        spans, context, target = inputs
        inside, weights = members(spans[0], spans[1], TOK_DEV)
        pooled = jnp.dot(inside, context.astype(jnp.float32), precision=lax.Precision.HIGHEST) * weights[:, None]
        residual = jnp.where((spans[1] > 0)[:, None], pooled - target.astype(jnp.float32), 0.0) * weights[:, None]
        return jnp.dot(jnp.transpose(inside), residual, precision=lax.Precision.HIGHEST).astype(jnp.bfloat16)

    grad_out = lax.map(student_rank, (student_spans, student_context.reshape(rank_count, TOK_DEV, DS), arrived))
    grad_out = grad_out.reshape(TOKENS, DS)
    return backward(student_query, student_keys, student_values, student_docs, HS, KVS, student_context, student_sums, grad_out)
```

```python
import functools

import jax
import jax.numpy as jnp
from jax import lax
from jax.experimental import pallas as pl
from jax.experimental.pallas import tpu as pltpu
from jax.sharding import PartitionSpec as P

HD = 128
ROWS = 160
SEQ = 32
TOKENS = ROWS * SEQ
SLOTS = 128
TG, TR = 2, 8
SR = 7
KV = 2 * TG * HD + 2 * HD
MESH = pl.DeviceIdType.MESH
SCALE = HD**-0.5
EXP2_SCALE = SCALE * 1.4426950408889634
LOW = -1e30
MASKED = -3e38
FB = 512
BB = 320
CHUNK = 256
VMEM_ALL = 60 * 1024 * 1024

NT = (((1,), (1,)), ((), ()))
TN = (((0,), (0,)), ((), ()))


def dot(a, b, dims=None):
    if dims is None:
        dims = (((1,), (0,)), ((), ()))
    return lax.dot_general(a, b, dims, preferred_element_type=jnp.float32)


def place():
    me = lax.axis_index("seq")
    return me, me // 8, (me // 2) % 4, me % 2


def seq_of(z, x, c):
    return (z * 4 + x) * 2 + c


def greet(peers):
    barrier = pltpu.get_barrier_semaphore()
    for peer in peers:
        pl.semaphore_signal(barrier, inc=1, device_id=peer, device_id_type=MESH)
    pl.semaphore_wait(barrier, len(peers))


GATHER_OPS = 71


def gather_kernel(tk, tv, sk, sv, gath, own_sem, send_sem, recv_sem):
    me, z, x, c = place()
    y = lax.axis_index("mp")

    locals_ = []
    at = 0
    for i, ref in enumerate((tk, tv, sk, sv)):
        width = ref.shape[1]
        copy = pltpu.make_async_copy(
            ref, gath.at[me, :, pl.ds(at, width)], own_sem.at[i]
        )
        copy.start()
        locals_.append(copy)
        at += width

    def node(half, p, q):
        zz, xx = (q, p) if half == 0 else (p, q)
        return seq_of(lax.rem(zz + 4, 4), lax.rem(xx + 4, 4), c)

    pos = ((x, z), (z, x))
    partner = seq_of(z, x, 1 - c)
    greet(
        [(node(0, x + 1, z), y), (node(0, x + 3, z), y)]
        + [(node(0, x, z + 1), y), (node(0, x, z + 3), y)]
        + [(partner, y)]
    )

    count = [0]
    started = []

    def send(slot, rows, cols, peer):
        i = count[0]
        count[0] += 1
        ref = gath.at[slot, pl.ds(*rows), pl.ds(*cols)]
        copy = pltpu.make_async_remote_copy(
            src_ref=ref,
            dst_ref=ref,
            send_sem=send_sem.at[i],
            recv_sem=recv_sem.at[i],
            device_id=(peer, y),
            device_id_type=MESH,
        )
        copy.start()
        started.append(copy)
        return i

    def arrive(i, slot, rows, cols):
        ref = gath.at[slot, pl.ds(*rows), pl.ds(*cols)]
        pltpu.make_async_remote_copy(
            src_ref=ref,
            dst_ref=ref,
            send_sem=send_sem.at[i],
            recv_sem=recv_sem.at[i],
            device_id=(partner, y),
            device_id_type=MESH,
        ).wait_recv()

    half_rows = ((0, ROWS // 2), (ROWS // 2, ROWS // 2))
    whole, left, right = (0, KV), (0, KV // 2), (KV // 2, KV // 2)
    died = []

    def die(slot_offset, rows):
        slot, theirs = slot_offset
        died.append((send(slot, rows, whole, partner), theirs, rows))

    def both_cores(half, dp, dq):
        p, q = pos[half]
        zz, xx = (q + dq, p + dp) if half == 0 else (p + dp, q + dq)
        zz, xx = lax.rem(zz + 4, 4), lax.rem(xx + 4, 4)
        return seq_of(zz, xx, c), seq_of(zz, xx, 1 - c)

    def mine(half, dp, dq):
        return both_cores(half, dp, dq)[0]

    def peer(half, dp, dq):
        return mine(half, dp, dq)

    for copy in locals_:
        copy.wait()

    first = {}
    second = {}
    for half in (0, 1):
        rows = half_rows[half]
        for d in (1, -1):
            first[half, d] = send(me, rows, whole, peer(half, d, 0))
    for half in (0, 1):
        rows = half_rows[half]
        for d in (1, -1):
            second[half, 0, d] = send(me, rows, whole, peer(half, 0, d))
    died.append((send(me, (0, ROWS), whole, partner), partner, (0, ROWS)))

    def spread(half, dp):
        rows = half_rows[half]
        for d in (1, -1):
            second[half, dp, d] = send(mine(half, dp, 0), rows, whole, peer(half, 0, d))
        die(both_cores(half, dp, 0), rows)

    across = {}
    for d, cols in ((1, left), (-1, right)):
        for half in (0, 1):
            rows = half_rows[half]
            arrive(first[half, d], mine(half, -d, 0), rows, whole)
            across[half, d] = send(mine(half, -d, 0), rows, cols, peer(half, d, 0))
            spread(half, -d)

    further = {}

    def pass_on(half, dp):
        rows = half_rows[half]
        for d, cols in ((1, left), (-1, right)):
            slot = mine(half, dp, -d)
            arrive(second[half, dp, d], slot, rows, whole)
            further[half, dp, d] = send(slot, rows, cols, peer(half, 0, d))
            die(both_cores(half, dp, -d), rows)

    for half in (0, 1):
        pass_on(half, 0)
    for half in (0, 1):
        rows = half_rows[half]
        for d, cols in ((1, left), (-1, right)):
            arrive(across[half, d], mine(half, -2 * d, 0), rows, cols)
        spread(half, 2)
    for dp in (-1, 1):
        for half in (0, 1):
            pass_on(half, dp)

    def ended(half, dp):
        rows = half_rows[half]
        for d, cols in ((1, left), (-1, right)):
            arrive(further[half, dp, d], mine(half, dp, -2 * d), rows, cols)
        die(both_cores(half, dp, 2), rows)

    for half in (0, 1):
        ended(half, 0)
    for half in (0, 1):
        pass_on(half, 2)
    for dp in (-1, 1, 2):
        for half in (0, 1):
            ended(half, dp)
    for i, slot, rows in died:
        arrive(i, slot, rows, whole)
    for copy in started:
        copy.wait_send()
    assert count[0] == GATHER_OPS, count[0]


def gather(tk, tv, sk, sv):
    hbm = pl.BlockSpec(memory_space=pl.ANY)
    return pl.pallas_call(
        gather_kernel,
        out_shape=jax.ShapeDtypeStruct((SEQ, ROWS, KV), jnp.bfloat16),
        in_specs=[hbm] * 4,
        out_specs=pl.BlockSpec(memory_space=pltpu.VMEM),
        scratch_shapes=[
            pltpu.SemaphoreType.DMA((4,)),
            pltpu.SemaphoreType.DMA((GATHER_OPS,)),
            pltpu.SemaphoreType.DMA((GATHER_OPS,)),
        ],
        compiler_params=pltpu.CompilerParams(
            collective_id=0, has_side_effects=True, vmem_limit_bytes=VMEM_ALL
        ),
        name="gather",
    )(tk, tv, sk, sv)


def doc_starts(docs_ref, positions, place_):
    bound = jnp.int32(0)
    starts = jnp.zeros_like(positions)
    lo = jnp.int32(0)
    hi = jnp.int32(0)
    for k in range(docs_ref.shape[0]):
        bound = bound + docs_ref[k]
        starts = jnp.where(bound <= positions, bound, starts)
        lo = jnp.where(bound <= place_, bound, lo)
        hi = jnp.where(bound <= place_ + ROWS - 1, bound, hi)
    return starts, lo, hi


def lane_rows(ratio):
    lane = lax.broadcasted_iota(jnp.int32, (1, ratio * ROWS), 1)
    cut = ratio * 128
    return jnp.where(lane < cut, lane & 127, 128 + ((lane - cut) & 31))


def stack_heads(dst, src, first_head, ratio):
    for h in range(ratio):
        cols = slice((first_head + h) * HD, (first_head + h + 1) * HD)
        dst[h * 128 : (h + 1) * 128, :] = src[0:128, cols]
        dst[ratio * 128 + h * 32 : ratio * 128 + (h + 1) * 32, :] = src[128:160, cols]


def chunks(width):
    return [(a, min(a + CHUNK, width)) for a in range(0, width, CHUNK)]


def attend(docs_ref, gath, q_stacks, k_cols, v_cols, m_refs, l_refs, acc_refs, ratio):
    place_ = lax.axis_index("seq") * ROWS
    positions = lane_rows(ratio) + place_
    starts, lo, hi = doc_starts(docs_ref, positions, place_)
    width = ratio * ROWS
    for m_ref, l_ref, acc_ref in zip(m_refs, l_refs, acc_refs):
        m_ref[...] = jnp.full(m_ref.shape, LOW, jnp.float32)
        l_ref[...] = jnp.zeros(l_ref.shape, jnp.float32)
        acc_ref[...] = jnp.zeros(acc_ref.shape, jnp.float32)
    begin = (lo // 16) * 16
    steps = (place_ + ROWS - begin + FB - 1) // FB

    def block(base, at, masked):
        for q, kc, vc, m_ref, l_ref, acc_ref in zip(
            q_stacks, k_cols, v_cols, m_refs, l_refs, acc_refs
        ):
            keys = gath[pl.ds(at, FB), kc : kc + HD]
            values_t = jnp.transpose(gath[pl.ds(at, FB), vc : vc + HD])
            for a, b in chunks(width):
                s = dot(keys, q[a:b, :], NT)
                if masked:
                    places = at + lax.broadcasted_iota(jnp.int32, (FB, b - a), 0)
                    lower = jnp.maximum(starts[:, a:b], base)
                    ok = (places >= lower) & (places <= positions[:, a:b])
                    s = jnp.where(ok, s, MASKED)
                m_old = m_ref[:, a:b]
                m_new = jnp.maximum(m_old, jnp.max(s, axis=0, keepdims=True))
                p = jnp.exp2((s - m_new) * EXP2_SCALE)
                alpha = jnp.exp2((m_old - m_new) * EXP2_SCALE)
                m_ref[:, a:b] = m_new
                l_ref[:, a:b] = l_ref[:, a:b] * alpha + jnp.sum(p, axis=0, keepdims=True)
                acc_ref[:, a:b] = acc_ref[:, a:b] * alpha + dot(
                    values_t, p.astype(jnp.bfloat16)
                )

    @pl.loop(0, steps)
    def _(step):
        base = pl.multiple_of(begin + step * FB, 16)
        at = pl.multiple_of(jnp.minimum(base, TOKENS - FB), 16)
        full = (base >= hi) & (base + FB - 1 <= place_)

        @pl.when(full)
        def _():
            block(base, at, False)

        @pl.when(jnp.logical_not(full))
        def _():
            block(base, at, True)


def member_rows(spans_ref):
    start = spans_ref[0, 0:1, :]
    length = spans_ref[0, 1:2, :]
    row = lax.broadcasted_iota(jnp.int32, (ROWS, SLOTS), 0)
    inside = (row >= start) & (row < start + length)
    weight = 1.0 / jnp.maximum(length, 1).astype(jnp.float32)
    return inside.astype(jnp.float32).astype(jnp.bfloat16), weight, length


def tail_members(member, ratio):
    tail = jnp.concatenate([member[128:160]] * ratio, axis=0)
    owner = lax.broadcasted_iota(jnp.int32, (ratio * 32, SLOTS), 0) // 32
    zero = jnp.zeros_like(tail)
    return [jnp.where(owner == h, tail, zero) for h in range(ratio)]


def pooled_head(context_t, member, tail, h, ratio):
    near = dot(context_t[:, h * 128 : (h + 1) * 128], member[0:128])
    return near + dot(context_t[:, ratio * 128 :], tail)


def forward_kernel(
    tdocs, sdocs, tq, sq, gath, tspans, pooled, sctx, slse,
    tstack, sstack, tm, tl, tacc, sm, sl, sacc,
):
    for g in range(TG):
        stack_heads(tstack.at[g], tq, g * TR, TR)
    stack_heads(sstack, sq, 0, SR)
    attend(
        tdocs,
        gath,
        [tstack.at[g] for g in range(TG)],
        [g * HD for g in range(TG)],
        [(TG + g) * HD for g in range(TG)],
        [tm.at[g] for g in range(TG)],
        [tl.at[g] for g in range(TG)],
        [tacc.at[g] for g in range(TG)],
        TR,
    )
    member, weight, _ = member_rows(tspans)
    tails = tail_members(member, TR)
    for g in range(TG):
        context_t = (tacc[g] / tl[g]).astype(jnp.bfloat16)
        for h in range(TR):
            sums = pooled_head(context_t, member, tails[h], h, TR) * weight
            cols = slice((g * TR + h) * HD, (g * TR + h + 1) * HD)
            pooled[:, cols] = jnp.transpose(sums).astype(jnp.bfloat16)
    attend(
        sdocs, gath, [sstack], [2 * TG * HD], [(2 * TG + 1) * HD], [sm], [sl], [sacc], SR
    )
    sctx[...] = (sacc[...] / sl[...]).astype(jnp.bfloat16)
    slse[...] = sm[...] * EXP2_SCALE + jnp.log2(sl[...])


def forward(tdocs, sdocs, tq, sq, gath, tspans):
    vmem = pl.BlockSpec(memory_space=pltpu.VMEM)
    smem = pl.BlockSpec(memory_space=pltpu.SMEM)
    tw, sw = TR * ROWS, SR * ROWS
    return pl.pallas_call(
        forward_kernel,
        out_shape=(
            jax.ShapeDtypeStruct((SLOTS, TG * TR * HD), jnp.bfloat16),
            jax.ShapeDtypeStruct((HD, sw), jnp.bfloat16),
            jax.ShapeDtypeStruct((1, sw), jnp.float32),
        ),
        in_specs=[smem, smem, vmem, vmem, vmem, vmem],
        out_specs=(vmem, vmem, vmem),
        scratch_shapes=[
            pltpu.VMEM((TG, tw, HD), jnp.bfloat16),
            pltpu.VMEM((sw, HD), jnp.bfloat16),
            pltpu.VMEM((TG, 1, tw), jnp.float32),
            pltpu.VMEM((TG, 1, tw), jnp.float32),
            pltpu.VMEM((TG, HD, tw), jnp.float32),
            pltpu.VMEM((1, sw), jnp.float32),
            pltpu.VMEM((1, sw), jnp.float32),
            pltpu.VMEM((HD, sw), jnp.float32),
        ],
        compiler_params=pltpu.CompilerParams(vmem_limit_bytes=VMEM_ALL),
        name="forward",
    )(tdocs, sdocs, tq, sq, gath, tspans)


def align_kernel(
    pooled, projector, arrived, wide, part, near, far, blocks, landed,
    load_sem, send_sem, recv_sem, a2a_send, a2a_recv, own_sem,
):
    me = lax.axis_index("seq")
    y = lax.axis_index("mp")
    cols = part.shape[2]
    half = SLOTS // 2
    up, down, across = lax.rem(y + 1, 4), lax.rem(y + 3, 4), lax.rem(y + 2, 4)
    order = (across, up, down, y)
    loads = []
    for i, target in enumerate(order):
        begin = pl.multiple_of(target * cols, 128)
        copy = pltpu.make_async_copy(
            projector.at[:, pl.ds(begin, cols)], wide.at[i], load_sem.at[i]
        )
        copy.start()
        loads.append(copy)

    barrier = pltpu.get_barrier_semaphore()
    for target in (up, down):
        pl.semaphore_signal(barrier, inc=1, device_id=(me, target), device_id_type=MESH)

    @pl.loop(1, SEQ)
    def _(k):
        pl.semaphore_signal(
            barrier, inc=1, device_id=(lax.rem(me + k, SEQ), y), device_id_type=MESH
        )

    pl.semaphore_wait(barrier, SEQ + 1)

    def project(i):
        loads[i].wait()
        return dot(pooled[...], wide[i])

    def remote(i, src, dst, target):
        return pltpu.make_async_remote_copy(
            src_ref=src,
            dst_ref=dst,
            send_sem=send_sem.at[i],
            recv_sem=recv_sem.at[i],
            device_id=(me, target),
            device_id_type=MESH,
        )

    low, high = pl.ds(0, half), pl.ds(half, half)
    hops = [
        remote(0, part.at[0, low], far.at[0], up),
        remote(1, part.at[0, high], far.at[1], down),
        remote(2, part.at[1, high], near.at[0, high], up),
        remote(3, part.at[2, low], near.at[1, low], down),
        remote(4, part.at[1, low], near.at[0, low], up),
        remote(5, part.at[2, high], near.at[1, high], down),
    ]
    part[0] = project(0).astype(jnp.bfloat16)
    hops[0].start()
    hops[1].start()
    for_up = project(1)
    part[1, half:] = for_up[half:].astype(jnp.bfloat16)
    hops[2].start()
    for_down = project(2)
    part[2, :half] = for_down[:half].astype(jnp.bfloat16)
    hops[3].start()
    hops[0].wait_recv()
    part[1, :half] = (for_up[:half] + far[0].astype(jnp.float32)).astype(jnp.bfloat16)
    hops[4].start()
    hops[1].wait_recv()
    part[2, half:] = (for_down[half:] + far[1].astype(jnp.float32)).astype(jnp.bfloat16)
    hops[5].start()
    mine = project(3)
    for i in (2, 3, 4, 5):
        hops[i].wait_recv()
    total = mine + near[0].astype(jnp.float32) + near[1].astype(jnp.float32)
    for d in range(SEQ):
        blocks[d] = total[4 * d : 4 * d + 4].astype(jnp.bfloat16)

    def exchange(k, src, target):
        return pltpu.make_async_remote_copy(
            src_ref=blocks.at[target],
            dst_ref=landed.at[src],
            send_sem=a2a_send.at[k],
            recv_sem=a2a_recv.at[k],
            device_id=(target, y),
            device_id_type=MESH,
        )

    @pl.loop(1, SEQ)
    def _(k):
        exchange(k, me, lax.rem(me + k, SEQ)).start()

    own = pltpu.make_async_copy(blocks.at[me], landed.at[me], own_sem)
    own.start()
    own.wait()

    @pl.loop(1, SEQ)
    def _(k):
        exchange(k, lax.rem(me + SEQ - k, SEQ), lax.rem(me + k, SEQ)).wait_recv()

    for s in range(SEQ):
        arrived[4 * s : 4 * s + 4, :] = landed[s].astype(jnp.float32)

    @pl.loop(1, SEQ)
    def _(k):
        exchange(k, me, lax.rem(me + k, SEQ)).wait_send()

    for hop in hops:
        hop.wait_send()


def align(pooled, projector):
    vmem = pl.BlockSpec(memory_space=pltpu.VMEM)
    depth, width = projector.shape
    cols = width // 4
    return pl.pallas_call(
        align_kernel,
        out_shape=jax.ShapeDtypeStruct((SLOTS, cols), jnp.float32),
        in_specs=[vmem, pl.BlockSpec(memory_space=pl.ANY)],
        out_specs=vmem,
        scratch_shapes=[
            pltpu.VMEM((4, depth, cols), jnp.bfloat16),
            pltpu.VMEM((3, SLOTS, cols), jnp.bfloat16),
            pltpu.VMEM((2, SLOTS, cols), jnp.bfloat16),
            pltpu.VMEM((2, SLOTS // 2, cols), jnp.bfloat16),
            pltpu.VMEM((SEQ, 4, cols), jnp.bfloat16),
            pltpu.VMEM((SEQ, 4, cols), jnp.bfloat16),
            pltpu.SemaphoreType.DMA((4,)),
            pltpu.SemaphoreType.DMA((6,)),
            pltpu.SemaphoreType.DMA((6,)),
            pltpu.SemaphoreType.DMA((SEQ,)),
            pltpu.SemaphoreType.DMA((SEQ,)),
            pltpu.SemaphoreType.DMA,
        ],
        compiler_params=pltpu.CompilerParams(
            collective_id=1, has_side_effects=True, vmem_limit_bytes=VMEM_ALL
        ),
        name="align",
    )(pooled, projector)


def backward_kernel(
    sdocs, sq, gath, sctx, slse, arrived, sspans, grad_q, terms,
    qstack, dstack, dq_t, delta_ref,
):
    place_ = lax.axis_index("seq") * ROWS
    width = SR * ROWS
    terms[...] = jnp.zeros(terms.shape, terms.dtype)
    dq_t[...] = jnp.zeros(dq_t.shape, jnp.float32)
    stack_heads(qstack, sq, 0, SR)
    member, weight, length = member_rows(sspans)
    tails = tail_members(member, SR)
    for h in range(SR):
        pooled_t = pooled_head(sctx, member, tails[h], h, SR) * weight
        target_t = jnp.transpose(arrived[:, h * HD : (h + 1) * HD])
        gap_t = jnp.where(length > 0, pooled_t - target_t, 0.0) * weight
        high = gap_t.astype(jnp.bfloat16)
        rest = (gap_t - high.astype(jnp.float32)).astype(jnp.bfloat16)
        dout = (dot(member, high, NT) + dot(member, rest, NT)).astype(jnp.bfloat16)
        dstack[h * 128 : (h + 1) * 128, :] = dout[0:128]
        dstack[SR * 128 + h * 32 : SR * 128 + (h + 1) * 32, :] = dout[128:160]
    for a, b in chunks(width):
        dout_t = jnp.transpose(dstack[a:b, :].astype(jnp.float32))
        delta_ref[:, a:b] = jnp.sum(
            dout_t * sctx[:, a:b].astype(jnp.float32), axis=0, keepdims=True
        )

    positions = lane_rows(SR) + place_
    starts, lo, hi = doc_starts(sdocs, positions, place_)
    kc, vc = 2 * TG * HD, (2 * TG + 1) * HD

    def block(at, masked):
        keys = gath[pl.ds(at, BB), kc : kc + HD]
        values = gath[pl.ds(at, BB), vc : vc + HD]
        keys_t = jnp.transpose(keys)
        grad_k = jnp.zeros((BB, HD), jnp.float32)
        grad_v = jnp.zeros((BB, HD), jnp.float32)
        for a, b in chunks(width):
            q = qstack[a:b, :]
            dout = dstack[a:b, :]
            s = dot(keys, q, NT)
            p = jnp.exp2(s * EXP2_SCALE - slse[:, a:b])
            if masked:
                places = at + lax.broadcasted_iota(jnp.int32, (BB, b - a), 0)
                ok = (places >= starts[:, a:b]) & (places <= positions[:, a:b])
                p = jnp.where(ok, p, 0.0)
            ds = (p * (dot(values, dout, NT) - delta_ref[:, a:b])).astype(jnp.bfloat16)
            grad_v = grad_v + dot(p.astype(jnp.bfloat16), dout)
            grad_k = grad_k + dot(ds, q)
            dq_t[:, a:b] = dq_t[:, a:b] + dot(keys_t, ds)
        terms[pl.ds(at, BB), 0:HD] = (grad_k * SCALE).astype(jnp.bfloat16)
        terms[pl.ds(at, BB), HD : 2 * HD] = grad_v.astype(jnp.bfloat16)

    @pl.loop(lo // BB, (place_ + ROWS - 1) // BB + 1)
    def _(step):
        at = pl.multiple_of(step * BB, BB)
        full = (at >= hi) & (at + BB - 1 <= place_)

        @pl.when(full)
        def _():
            block(at, False)

        @pl.when(jnp.logical_not(full))
        def _():
            block(at, True)

    for h in range(SR):
        cols = slice(h * HD, (h + 1) * HD)
        grad_q[0:128, cols] = (jnp.transpose(dq_t[:, h * 128 : (h + 1) * 128]) * SCALE).astype(
            jnp.bfloat16
        )
    rest = (jnp.transpose(dq_t[:, SR * 128 :]) * SCALE).astype(jnp.bfloat16)
    for h in range(SR):
        grad_q[128:160, h * HD : (h + 1) * HD] = rest[h * 32 : (h + 1) * 32]


def backward(sdocs, sq, gath, sctx, slse, arrived, sspans):
    vmem = pl.BlockSpec(memory_space=pltpu.VMEM)
    smem = pl.BlockSpec(memory_space=pltpu.SMEM)
    sw = SR * ROWS
    return pl.pallas_call(
        backward_kernel,
        out_shape=(
            jax.ShapeDtypeStruct((ROWS, SR * HD), jnp.bfloat16),
            jax.ShapeDtypeStruct((TOKENS, 2 * HD), jnp.bfloat16),
        ),
        in_specs=[smem, vmem, vmem, vmem, vmem, vmem, vmem],
        out_specs=(vmem, vmem),
        scratch_shapes=[
            pltpu.VMEM((sw, HD), jnp.bfloat16),
            pltpu.VMEM((sw, HD), jnp.bfloat16),
            pltpu.VMEM((HD, sw), jnp.float32),
            pltpu.VMEM((1, sw), jnp.float32),
        ],
        compiler_params=pltpu.CompilerParams(vmem_limit_bytes=VMEM_ALL),
        name="backward",
    )(sdocs, sq, gath, sctx, slse, arrived, sspans)


def scatter_kernel(
    terms, grad_k, grad_v, theirs, chip, far1, near1, out1, far2, near2,
    die_send, die_recv, send_sem, recv_sem,
):
    me, z, x, c = place()
    y = lax.axis_index("mp")
    partner = seq_of(z, x, 1 - c)
    wrap = lambda v: lax.rem(v + 4, 4)

    def peer(axis, d):
        return seq_of(wrap(z + d), x, c) if axis == "z" else seq_of(z, wrap(x + d), c)

    greet(
        [(peer("z", 1), y), (peer("z", 3), y), (peer("x", 1), y), (peer("x", 3), y)]
        + [(partner, y)]
    )

    def crossing(i):
        return pltpu.make_async_remote_copy(
            src_ref=terms.at[pl.ds(4 * i, 4), 1 - c],
            dst_ref=theirs.at[pl.ds(4 * i, 4)],
            send_sem=die_send.at[i],
            recv_sem=die_recv.at[i],
            device_id=(partner, y),
            device_id_type=MESH,
        )

    for i in range(4):
        crossing(i).start()

    def remote(i, src, dst, target):
        return pltpu.make_async_remote_copy(
            src_ref=src,
            dst_ref=dst,
            send_sem=send_sem.at[i],
            recv_sem=recv_sem.at[i],
            device_id=(target, y),
            device_id_type=MESH,
        )

    for i in range(4):
        crossing(i).wait_recv()
        part = pl.ds(4 * i, 4)
        both = terms[part, c].astype(jnp.float32) + theirs[part].astype(jnp.float32)
        low = both.astype(jnp.bfloat16)
        chip[0, i] = low[:, 0:80]
        for j in range(4):
            chip[1, j, i] = low[j, 80:160]

    f32 = lambda v: v.astype(jnp.float32)
    all_hops = []
    axes = (("z", "x"), ("x", "z"))
    pos = ((z, x), (x, z))
    first = []
    for h in (0, 1):
        axis = axes[h][0]
        p = pos[h][0]
        up, down = peer(axis, 1), peer(axis, 3)
        to_far, to_up, to_down = wrap(p + 2), wrap(p + 1), wrap(p + 3)
        lo, hi = pl.ds(0, 2), pl.ds(2, 2)
        hops = [
            remote(12 * h + 0, chip.at[h, to_far, lo], far1.at[h, 0], up),
            remote(12 * h + 1, chip.at[h, to_far, hi], far1.at[h, 1], down),
            remote(12 * h + 2, chip.at[h, to_up, hi], near1.at[h, 0, hi], up),
            remote(12 * h + 3, chip.at[h, to_down, lo], near1.at[h, 1, lo], down),
            remote(12 * h + 4, chip.at[h, to_up, lo], near1.at[h, 0, lo], up),
            remote(12 * h + 5, chip.at[h, to_down, hi], near1.at[h, 1, hi], down),
        ]
        for k in range(4):
            hops[k].start()
        first.append((hops, to_up, to_down))
        all_hops += hops
    for h in (0, 1):
        hops, to_up, to_down = first[h]
        lo, hi = pl.ds(0, 2), pl.ds(2, 2)
        hops[0].wait_recv()
        chip[h, to_up, lo] = (f32(chip[h, to_up, lo]) + f32(far1[h, 0])).astype(jnp.bfloat16)
        hops[4].start()
        hops[1].wait_recv()
        chip[h, to_down, hi] = (f32(chip[h, to_down, hi]) + f32(far1[h, 1])).astype(jnp.bfloat16)
        hops[5].start()
    second = []
    for h in (0, 1):
        hops = first[h][0]
        for k in range(2, 6):
            hops[k].wait_recv()
        out1[h] = (f32(chip[h, pos[h][0]]) + f32(near1[h, 0]) + f32(near1[h, 1])).astype(
            jnp.bfloat16
        )
        axis = axes[h][1]
        p = pos[h][1]
        up, down = peer(axis, 1), peer(axis, 3)
        to_far, to_up, to_down = wrap(p + 2), wrap(p + 1), wrap(p + 3)
        lo, hi = pl.ds(0, HD), pl.ds(HD, HD)
        rows = pl.ds(0, 80)
        hops = [
            remote(12 * h + 6, out1.at[h, to_far, rows, lo], far2.at[h, 0], up),
            remote(12 * h + 7, out1.at[h, to_far, rows, hi], far2.at[h, 1], down),
            remote(12 * h + 8, out1.at[h, to_up, rows, hi], near2.at[h, 0, rows, hi], up),
            remote(12 * h + 9, out1.at[h, to_down, rows, lo], near2.at[h, 1, rows, lo], down),
            remote(12 * h + 10, out1.at[h, to_up, rows, lo], near2.at[h, 0, rows, lo], up),
            remote(12 * h + 11, out1.at[h, to_down, rows, hi], near2.at[h, 1, rows, hi], down),
        ]
        for k in range(4):
            hops[k].start()
        second.append((hops, to_up, to_down))
        all_hops += hops
    for h in (0, 1):
        hops, to_up, to_down = second[h]
        hops[0].wait_recv()
        out1[h, to_up, :, 0:HD] = (f32(out1[h, to_up, :, 0:HD]) + f32(far2[h, 0])).astype(
            jnp.bfloat16
        )
        hops[4].start()
        hops[1].wait_recv()
        out1[h, to_down, :, HD:] = (f32(out1[h, to_down, :, HD:]) + f32(far2[h, 1])).astype(
            jnp.bfloat16
        )
        hops[5].start()
    for h in (0, 1):
        hops = second[h][0]
        for k in range(2, 6):
            hops[k].wait_recv()
        total = (
            f32(out1[h, pos[h][1]]) + f32(near2[h, 0]) + f32(near2[h, 1])
        ).astype(jnp.bfloat16)
        grad_k[80 * h : 80 * h + 80, :] = total[:, 0:HD]
        grad_v[80 * h : 80 * h + 80, :] = total[:, HD:]
    for hop in all_hops:
        hop.wait_send()
    for i in range(4):
        crossing(i).wait_send()


def scatter(terms):
    vmem = pl.BlockSpec(memory_space=pltpu.VMEM)
    bf16 = jnp.bfloat16
    width = terms.shape[-1]
    return pl.pallas_call(
        scatter_kernel,
        out_shape=(
            jax.ShapeDtypeStruct((ROWS, HD), bf16),
            jax.ShapeDtypeStruct((ROWS, HD), bf16),
        ),
        in_specs=[vmem],
        out_specs=(vmem, vmem),
        scratch_shapes=[
            pltpu.VMEM((16, ROWS, width), bf16),
            pltpu.VMEM((2, 4, 4, 80, width), bf16),
            pltpu.VMEM((2, 2, 2, 80, width), bf16),
            pltpu.VMEM((2, 2, 4, 80, width), bf16),
            pltpu.VMEM((2, 4, 80, width), bf16),
            pltpu.VMEM((2, 2, 80, HD), bf16),
            pltpu.VMEM((2, 2, 80, width), bf16),
            pltpu.SemaphoreType.DMA((4,)),
            pltpu.SemaphoreType.DMA((4,)),
            pltpu.SemaphoreType.DMA((24,)),
            pltpu.SemaphoreType.DMA((24,)),
        ],
        compiler_params=pltpu.CompilerParams(
            collective_id=2, has_side_effects=True, vmem_limit_bytes=VMEM_ALL
        ),
        name="scatter",
    )(terms)


def body(
    teacher_query,
    teacher_keys,
    teacher_values,
    teacher_docs,
    student_query,
    student_keys,
    student_values,
    student_docs,
    projector,
    teacher_spans,
    student_spans,
):
    gath = gather(teacher_keys, teacher_values, student_keys, student_values)
    gath = gath.reshape(TOKENS, KV)
    pooled, sctx, slse = forward(
        teacher_docs, student_docs, teacher_query, student_query, gath, teacher_spans
    )
    arrived = align(pooled, projector)
    grad_q, terms = backward(
        student_docs, student_query, gath, sctx, slse, arrived, student_spans
    )
    grad_k, grad_v = scatter(terms.reshape(16, 2, ROWS, 2 * HD))
    return grad_q, grad_k, grad_v


def solution(mesh):
    return jax.shard_map(
        body,
        mesh=mesh,
        in_specs=(
            P("seq", "mp"),
            P("seq", "mp"),
            P("seq", "mp"),
            P(),
            P("seq", "mp"),
            P("seq", "mp"),
            P("seq", "mp"),
            P(),
            P("mp", None),
            P("seq", None, None),
            P("seq", None, None),
        ),
        out_specs=(P("seq", "mp"), P("seq", "mp"), P("seq", "mp")),
        check_vma=False,
    )
```

```python
import functools

import jax
import jax.numpy as jnp
from jax import lax
from jax.experimental import pallas as pl
from jax.experimental.pallas import tpu as pltpu
from jax.sharding import PartitionSpec as P

HD = 128
ROWS = 160
SEQ = 32
TOKENS = ROWS * SEQ
SLOTS = 128
TG, TR = 2, 8
SR = 7
KV = 2 * TG * HD + 2 * HD
MESH = pl.DeviceIdType.MESH
SCALE = HD**-0.5
EXP2_SCALE = SCALE * 1.4426950408889634
LOW = -1e30
MASKED = -3e38
NDOCS = 16
ONES, FLAG = NDOCS, NDOCS + 3
FAR = 1 << 20
FB = 512
BB = 512
CHUNK = 1280
VMEM_ALL = 60 * 1024 * 1024

NT = (((1,), (1,)), ((), ()))
TN = (((0,), (0,)), ((), ()))


def dot(a, b, dims=None):
    if dims is None:
        dims = (((1,), (0,)), ((), ()))
    return lax.dot_general(a, b, dims, preferred_element_type=jnp.float32)


def place():
    me = lax.axis_index("seq")
    return me, me // 8, (me // 2) % 4, me % 2


def seq_of(z, x, c):
    return (z * 4 + x) * 2 + c


def greet(peers):
    barrier = pltpu.get_barrier_semaphore()
    for peer in peers:
        pl.semaphore_signal(barrier, inc=1, device_id=peer, device_id_type=MESH)
    pl.semaphore_wait(barrier, len(peers))


GATHER_OPS = 71


def gather_kernel(tk, tv, sk, sv, gath, own_sem, send_sem, recv_sem):
    me, z, x, c = place()
    y = lax.axis_index("mp")

    locals_ = []
    at = 0
    for i, ref in enumerate((tk, tv, sk, sv)):
        width = ref.shape[1]
        copy = pltpu.make_async_copy(
            ref, gath.at[me, :, pl.ds(at, width)], own_sem.at[i]
        )
        copy.start()
        locals_.append(copy)
        at += width

    def node(half, p, q):
        zz, xx = (q, p) if half == 0 else (p, q)
        return seq_of(lax.rem(zz + 4, 4), lax.rem(xx + 4, 4), c)

    pos = ((x, z), (z, x))
    partner = seq_of(z, x, 1 - c)
    greet(
        [(node(0, x + 1, z), y), (node(0, x + 3, z), y)]
        + [(node(0, x, z + 1), y), (node(0, x, z + 3), y)]
        + [(partner, y)]
    )

    count = [0]
    started = []

    def send(slot, rows, cols, peer):
        i = count[0]
        count[0] += 1
        ref = gath.at[slot, pl.ds(*rows), pl.ds(*cols)]
        copy = pltpu.make_async_remote_copy(
            src_ref=ref,
            dst_ref=ref,
            send_sem=send_sem.at[i],
            recv_sem=recv_sem.at[i],
            device_id=(peer, y),
            device_id_type=MESH,
        )
        copy.start()
        started.append(copy)
        return i

    def arrive(i, slot, rows, cols):
        ref = gath.at[slot, pl.ds(*rows), pl.ds(*cols)]
        pltpu.make_async_remote_copy(
            src_ref=ref,
            dst_ref=ref,
            send_sem=send_sem.at[i],
            recv_sem=recv_sem.at[i],
            device_id=(partner, y),
            device_id_type=MESH,
        ).wait_recv()

    half_rows = ((0, ROWS // 2), (ROWS // 2, ROWS // 2))
    whole, left, right = (0, KV), (0, KV // 2), (KV // 2, KV // 2)
    died = []

    def die(slot_offset, rows):
        slot, theirs = slot_offset
        died.append((send(slot, rows, whole, partner), theirs, rows))

    def both_cores(half, dp, dq):
        p, q = pos[half]
        zz, xx = (q + dq, p + dp) if half == 0 else (p + dp, q + dq)
        zz, xx = lax.rem(zz + 4, 4), lax.rem(xx + 4, 4)
        return seq_of(zz, xx, c), seq_of(zz, xx, 1 - c)

    def mine(half, dp, dq):
        return both_cores(half, dp, dq)[0]

    def peer(half, dp, dq):
        return mine(half, dp, dq)

    for copy in locals_:
        copy.wait()

    first = {}
    second = {}
    for half in (0, 1):
        rows = half_rows[half]
        for d in (1, -1):
            first[half, d] = send(me, rows, whole, peer(half, d, 0))
    for half in (0, 1):
        rows = half_rows[half]
        for d in (1, -1):
            second[half, 0, d] = send(me, rows, whole, peer(half, 0, d))
    died.append((send(me, (0, ROWS), whole, partner), partner, (0, ROWS)))

    def spread(half, dp):
        rows = half_rows[half]
        for d in (1, -1):
            second[half, dp, d] = send(mine(half, dp, 0), rows, whole, peer(half, 0, d))
        die(both_cores(half, dp, 0), rows)

    across = {}
    for d, cols in ((1, left), (-1, right)):
        for half in (0, 1):
            rows = half_rows[half]
            arrive(first[half, d], mine(half, -d, 0), rows, whole)
            across[half, d] = send(mine(half, -d, 0), rows, cols, peer(half, d, 0))
            spread(half, -d)

    further = {}

    def pass_on(half, dp):
        rows = half_rows[half]
        for d, cols in ((1, left), (-1, right)):
            slot = mine(half, dp, -d)
            arrive(second[half, dp, d], slot, rows, whole)
            further[half, dp, d] = send(slot, rows, cols, peer(half, 0, d))
            die(both_cores(half, dp, -d), rows)

    for half in (0, 1):
        pass_on(half, 0)
    for half in (0, 1):
        rows = half_rows[half]
        for d, cols in ((1, left), (-1, right)):
            arrive(across[half, d], mine(half, -2 * d, 0), rows, cols)
        spread(half, 2)
    for dp in (-1, 1):
        for half in (0, 1):
            pass_on(half, dp)

    def ended(half, dp):
        rows = half_rows[half]
        for d, cols in ((1, left), (-1, right)):
            arrive(further[half, dp, d], mine(half, dp, -2 * d), rows, cols)
        die(both_cores(half, dp, 2), rows)

    for half in (0, 1):
        ended(half, 0)
    for half in (0, 1):
        pass_on(half, 2)
    for dp in (-1, 1, 2):
        for half in (0, 1):
            ended(half, dp)
    for i, slot, rows in died:
        arrive(i, slot, rows, whole)
    for copy in started:
        copy.wait_send()
    assert count[0] == GATHER_OPS, count[0]


def gather(tk, tv, sk, sv):
    hbm = pl.BlockSpec(memory_space=pl.ANY)
    return pl.pallas_call(
        gather_kernel,
        out_shape=jax.ShapeDtypeStruct((SEQ, ROWS, KV), jnp.bfloat16),
        in_specs=[hbm] * 4,
        out_specs=pl.BlockSpec(memory_space=pltpu.VMEM),
        scratch_shapes=[
            pltpu.SemaphoreType.DMA((4,)),
            pltpu.SemaphoreType.DMA((GATHER_OPS,)),
            pltpu.SemaphoreType.DMA((GATHER_OPS,)),
        ],
        compiler_params=pltpu.CompilerParams(
            collective_id=0, has_side_effects=True, vmem_limit_bytes=VMEM_ALL
        ),
        name="gather",
    )(tk, tv, sk, sv)


def doc_lanes(docs_ref):
    lane = lax.broadcasted_iota(jnp.int32, (1, 128), 1)
    first = jnp.where((lane >= ONES) & (lane < FLAG), -1, FAR)
    last = jnp.full((1, 128), FAR, jnp.int32)
    bound = jnp.int32(0)
    for k in range(NDOCS):
        first = jnp.where(lane == k, bound, first)
        bound = bound + docs_ref[k]
        last = jnp.where(lane == k, bound, last)
    return lane, first, last


def first_start(docs_ref, place_):
    bound = jnp.int32(0)
    lo = jnp.int32(0)
    for k in range(NDOCS):
        bound = bound + docs_ref[k]
        lo = jnp.where(bound <= place_, bound, lo)
    return lo


def key_marks(at, count, limit, lanes):
    lane, first, last = lanes
    first = jnp.where(lane == FLAG, limit, first)
    places = at + lax.broadcasted_iota(jnp.int32, (count, 128), 0)
    inside = (places >= first) & (places < last)
    return inside.astype(jnp.float32).astype(jnp.bfloat16)


def stack_heads(dst, src, first_head, ratio):
    for h in range(ratio):
        cols = slice((first_head + h) * HD, (first_head + h + 1) * HD)
        dst[h * 128 : (h + 1) * 128, 0:HD] = src[0:128, cols]
        dst[ratio * 128 + h * 32 : ratio * 128 + (h + 1) * 32, 0:HD] = src[128:160, cols]


def parts(value):
    high = value.astype(jnp.bfloat16).astype(jnp.float32)
    rest = value - high
    middle = rest.astype(jnp.bfloat16).astype(jnp.float32)
    return high, middle, rest - middle


def query_marks(places, shift, lanes):
    lane, first, last = lanes
    inside = (places >= first) & (places < last)
    marks = jnp.where((lane < NDOCS) & jnp.logical_not(inside) | (lane == FLAG), LOW, 0.0)
    for k, part in enumerate(parts(-shift)):
        marks = jnp.where(lane == ONES + k, part, marks)
    return marks.astype(jnp.bfloat16)


def mark_queries(dst, keys, place_, lanes, ratio):
    for begin, count, base in ((0, 128, 0), (128, 32, ratio * 128)):
        own = keys[begin : begin + count, :].astype(jnp.float32)
        places = place_ + begin + lax.broadcasted_iota(jnp.int32, (count, 1), 0)
        for h in range(ratio):
            rows = slice(base + h * count, base + (h + 1) * count)
            q = dst[rows, 0:HD].astype(jnp.float32)
            shift = jnp.sum(q * own, axis=1, keepdims=True)
            dst[rows, HD:] = query_marks(places, shift, lanes)


def lane_rows(ratio):
    lane = lax.broadcasted_iota(jnp.int32, (1, ratio * ROWS), 1)
    cut = ratio * 128
    return jnp.where(lane < cut, lane & 127, 128 + ((lane - cut) & 31))


def chunks(width):
    return [(a, min(a + CHUNK, width)) for a in range(0, width, CHUNK)]


def own_pairs(a, b, lanes_row):
    return lax.broadcasted_iota(jnp.int32, (ROWS, b - a), 0) <= lanes_row[:, a:b]


class Window:
    def __init__(self, docs_ref, gath, first_col, own, blocks, own_sem, sems, size):
        self.place = lax.axis_index("seq") * ROWS
        self.lo = first_start(docs_ref, self.place)
        self.size = size
        self.gath, self.own, self.blocks = gath, own, blocks
        self.own_sem, self.sems = own_sem, sems
        self.cols = pl.ds(first_col, own.shape[1])
        self.steps = (jnp.maximum(self.place - self.lo, 0) + size - 1) // size
        self.lanes = doc_lanes(docs_ref)

    def at(self, step):
        return pl.multiple_of(jnp.maximum(self.place - (step + 1) * self.size, 0), 16)

    def own_copy(self):
        rows = pl.ds(pl.multiple_of(self.place, 16), ROWS)
        return pltpu.make_async_copy(self.gath.at[rows, self.cols], self.own, self.own_sem)

    def copy(self, step):
        rows = pl.ds(self.at(step), self.size)
        return pltpu.make_async_copy(
            self.gath.at[rows, self.cols], self.blocks.at[step], self.sems.at[step]
        )

    def start(self):
        self.own_copy().start()

        @pl.loop(0, self.steps)
        def _(step):
            self.copy(step).start()

    def marks(self, step):
        return key_marks(
            self.at(step), self.size, self.place - step * self.size, self.lanes
        )

    def own_marks(self):
        return key_marks(self.place, ROWS, jnp.int32(FAR), self.lanes)


def extended(values):
    ones = jnp.ones((16, values.shape[0]), jnp.bfloat16)
    return jnp.concatenate([jnp.transpose(values), ones], axis=0)


def attend(window, q_refs, l_ref, acc_ref, top_ref, ratio):
    groups = len(q_refs)
    width = ratio * ROWS
    lanes_row = lane_rows(ratio)
    top_ref[...] = jnp.zeros(top_ref.shape, jnp.float32)

    def scores(g, keys, a, b, own):
        s = dot(keys, q_refs[g][a:b, :], NT)
        return jnp.where(own_pairs(a, b, lanes_row), s, MASKED) if own else s

    def block(kv, marks, own):
        for g in range(groups):
            keys = jnp.concatenate([kv[:, g * HD : (g + 1) * HD], marks], axis=1)
            values_t = extended(kv[:, (groups + g) * HD : (groups + g + 1) * HD])
            for a, b in chunks(width):
                p = jnp.exp2(scores(g, keys, a, b, own) * EXP2_SCALE)
                add = dot(values_t, p.astype(jnp.bfloat16))
                if l_ref is not None:
                    total = jnp.sum(p.reshape(p.shape[0] // 8, 8, b - a), axis=0)
                    l_ref[g, :, a:b] = total if own else l_ref[g, :, a:b] + total
                acc_ref[g, :, a:b] = add if own else acc_ref[g, :, a:b] + add

    def safe_block(kv, marks, own):
        for g in range(groups):
            keys = jnp.concatenate([kv[:, g * HD : (g + 1) * HD], marks], axis=1)
            values_t = extended(kv[:, (groups + g) * HD : (groups + g + 1) * HD])
            for a, b in chunks(width):
                s = scores(g, keys, a, b, own)
                old = jnp.full((1, b - a), LOW) if own else top_ref[g, :, a:b]
                new = jnp.maximum(old, jnp.max(s, axis=0, keepdims=True))
                p = jnp.exp2((s - new) * EXP2_SCALE)
                add = dot(values_t, p.astype(jnp.bfloat16))
                top_ref[g, :, a:b] = new
                alpha = None if own else jnp.exp2((old - new) * EXP2_SCALE)
                if l_ref is not None:
                    total = jnp.sum(p.reshape(p.shape[0] // 8, 8, b - a), axis=0)
                    l_ref[g, :, a:b] = total if own else l_ref[g, :, a:b] * alpha + total
                acc_ref[g, :, a:b] = add if own else acc_ref[g, :, a:b] * alpha + add

    block(window.own, window.own_marks(), True)

    @pl.loop(0, window.steps)
    def _(step):
        window.copy(step).wait()
        block(window.blocks.at[step], window.marks(step), False)

    @pl.when(jnp.logical_not(jnp.max(acc_ref[:, HD : HD + 8, :]) < 2.0**100))
    def _():
        safe_block(window.own, window.own_marks(), True)

        @pl.loop(0, window.steps)
        def _(step):
            safe_block(window.blocks.at[step], window.marks(step), False)


def member_rows(spans_ref):
    start = spans_ref[0, 0:1, :]
    length = spans_ref[0, 1:2, :]
    row = lax.broadcasted_iota(jnp.int32, (ROWS, SLOTS), 0)
    inside = (row >= start) & (row < start + length)
    weight = 1.0 / jnp.maximum(length, 1).astype(jnp.float32)
    return inside.astype(jnp.float32), weight, length


def forward_kernel(
    tdocs, sdocs, tq, sq, gath, tspans, pooled, sctx, qback,
    tstack, sstack, town, sown, tblocks, sblocks, tacc, ttop, sl, sacc, stop,
    own_sem, tsem, ssem,
):
    tcols, scols = 2 * TG * HD, 2 * HD
    twin = Window(tdocs, gath, 0, town, tblocks, own_sem.at[0], tsem, FB)
    swin = Window(sdocs, gath, tcols, sown, sblocks, own_sem.at[1], ssem, FB)
    twin.start()
    swin.start()
    for g in range(TG):
        stack_heads(tstack.at[g], tq, g * TR, TR)
    stack_heads(sstack, sq, 0, SR)
    twin.own_copy().wait()
    for g in range(TG):
        mark_queries(
            tstack.at[g], town.at[:, g * HD : (g + 1) * HD], twin.place, twin.lanes, TR
        )
    swin.own_copy().wait()
    mark_queries(sstack, sown.at[:, 0:HD], swin.place, swin.lanes, SR)

    attend(twin, [tstack.at[g] for g in range(TG)], None, tacc, ttop, TR)
    attend(swin, [sstack], sl, sacc, stop, SR)

    member, weight, _ = member_rows(tspans)
    member = member.astype(jnp.bfloat16)
    tail = jnp.concatenate([member[128:160]] * TR, axis=0)
    owner = lax.broadcasted_iota(jnp.int32, (TR * 32, SLOTS), 0) // 32
    for g in range(TG):
        inverse = 1.0 / tacc[g, HD : HD + 1]
        context_t = (tacc[g, 0:HD] * inverse).astype(jnp.bfloat16)
        for h in range(TR):
            sums = dot(context_t[:, h * 128 : (h + 1) * 128], member[0:128]) + dot(
                context_t[:, TR * 128 :], jnp.where(owner == h, tail, jnp.zeros_like(tail))
            )
            cols = slice((g * TR + h) * HD, (g * TR + h + 1) * HD)
            pooled[:, cols] = jnp.transpose(sums * weight).astype(jnp.bfloat16)

    total = jnp.sum(sl[0], axis=0, keepdims=True)
    inverse = 1.0 / sacc[0, HD : HD + 1]
    extra = stop[0] + jnp.log2(total) * (1.0 / EXP2_SCALE)
    for h in range(SR):
        cols = slice(h * 128, (h + 1) * 128)
        sctx[0:128, cols] = jnp.transpose(sacc[0, 0:HD, cols] * inverse[:, cols]).astype(
            jnp.bfloat16
        )
    rest = jnp.transpose(sacc[0, 0:HD, SR * 128 :] * inverse[:, SR * 128 :]).astype(jnp.bfloat16)
    for h in range(SR):
        sctx[128:160, h * HD : (h + 1) * HD] = rest[h * 32 : (h + 1) * 32]
    qback[:, 0:HD] = sstack[:, 0:HD]
    lane = swin.lanes[0]
    for a in range(0, SR * ROWS, 128):
        b = min(a + 128, SR * ROWS)
        column = jnp.transpose(jnp.broadcast_to(extra[:, a:b], (8, b - a)))[:, 0:1]
        marks = sstack[a:b, HD:].astype(jnp.float32)
        ones = (lane >= ONES) & (lane < FLAG)
        before = jnp.sum(jnp.where(ones, marks, 0.0), axis=1, keepdims=True)
        for k, part in enumerate(parts(before - column)):
            marks = jnp.where(lane == ONES + k, part, marks)
        qback[a:b, HD:] = marks.astype(jnp.bfloat16)


def forward(tdocs, sdocs, tq, sq, gath, tspans):
    vmem = pl.BlockSpec(memory_space=pltpu.VMEM)
    smem = pl.BlockSpec(memory_space=pltpu.SMEM)
    hbm = pl.BlockSpec(memory_space=pl.ANY)
    tw, sw = TR * ROWS, SR * ROWS
    bf16, f32 = jnp.bfloat16, jnp.float32
    return pl.pallas_call(
        forward_kernel,
        out_shape=(
            jax.ShapeDtypeStruct((SLOTS, TG * TR * HD), bf16),
            jax.ShapeDtypeStruct((ROWS, SR * HD), bf16),
            jax.ShapeDtypeStruct((sw, 2 * HD), bf16),
        ),
        in_specs=[smem, smem, vmem, vmem, hbm, vmem],
        out_specs=(vmem, vmem, vmem),
        scratch_shapes=[
            pltpu.VMEM((TG, tw, 2 * HD), bf16),
            pltpu.VMEM((sw, 2 * HD), bf16),
            pltpu.VMEM((ROWS, 2 * TG * HD), bf16),
            pltpu.VMEM((ROWS, 2 * HD), bf16),
            pltpu.VMEM((TOKENS // FB, FB, 2 * TG * HD), bf16),
            pltpu.VMEM((TOKENS // FB, FB, 2 * HD), bf16),
            pltpu.VMEM((TG, HD + 16, tw), f32),
            pltpu.VMEM((TG, 1, tw), f32),
            pltpu.VMEM((1, 8, sw), f32),
            pltpu.VMEM((1, HD + 16, sw), f32),
            pltpu.VMEM((1, 1, sw), f32),
            pltpu.SemaphoreType.DMA((2,)),
            pltpu.SemaphoreType.DMA((TOKENS // FB,)),
            pltpu.SemaphoreType.DMA((TOKENS // FB,)),
        ],
        compiler_params=pltpu.CompilerParams(vmem_limit_bytes=VMEM_ALL),
        name="forward",
    )(tdocs, sdocs, tq, sq, gath, tspans)


def align_kernel(
    pooled, projector, arrived, wide, part, near, far, blocks, landed,
    load_sem, send_sem, recv_sem, a2a_send, a2a_recv, own_sem,
):
    me = lax.axis_index("seq")
    y = lax.axis_index("mp")
    cols = part.shape[2]
    half = SLOTS // 2
    up, down, across = lax.rem(y + 1, 4), lax.rem(y + 3, 4), lax.rem(y + 2, 4)
    order = (across, up, down, y)
    loads = []
    for i, target in enumerate(order):
        begin = pl.multiple_of(target * cols, 128)
        copy = pltpu.make_async_copy(
            projector.at[:, pl.ds(begin, cols)], wide.at[i], load_sem.at[i]
        )
        copy.start()
        loads.append(copy)

    barrier = pltpu.get_barrier_semaphore()
    for target in (up, down):
        pl.semaphore_signal(barrier, inc=1, device_id=(me, target), device_id_type=MESH)

    @pl.loop(1, SEQ)
    def _(k):
        pl.semaphore_signal(
            barrier, inc=1, device_id=(lax.rem(me + k, SEQ), y), device_id_type=MESH
        )

    pl.semaphore_wait(barrier, SEQ + 1)

    def project(i):
        loads[i].wait()
        return dot(pooled[...], wide[i])

    def remote(i, src, dst, target):
        return pltpu.make_async_remote_copy(
            src_ref=src,
            dst_ref=dst,
            send_sem=send_sem.at[i],
            recv_sem=recv_sem.at[i],
            device_id=(me, target),
            device_id_type=MESH,
        )

    low, high = pl.ds(0, half), pl.ds(half, half)
    hops = [
        remote(0, part.at[0, low], far.at[0], up),
        remote(1, part.at[0, high], far.at[1], down),
        remote(2, part.at[1, high], near.at[0, high], up),
        remote(3, part.at[2, low], near.at[1, low], down),
        remote(4, part.at[1, low], near.at[0, low], up),
        remote(5, part.at[2, high], near.at[1, high], down),
    ]
    part[0] = project(0).astype(jnp.bfloat16)
    hops[0].start()
    hops[1].start()
    for_up = project(1)
    part[1, half:] = for_up[half:].astype(jnp.bfloat16)
    hops[2].start()
    for_down = project(2)
    part[2, :half] = for_down[:half].astype(jnp.bfloat16)
    hops[3].start()
    hops[0].wait_recv()
    part[1, :half] = (for_up[:half] + far[0].astype(jnp.float32)).astype(jnp.bfloat16)
    hops[4].start()
    hops[1].wait_recv()
    part[2, half:] = (for_down[half:] + far[1].astype(jnp.float32)).astype(jnp.bfloat16)
    hops[5].start()
    mine = project(3)
    for i in (2, 3, 4, 5):
        hops[i].wait_recv()
    total = mine + near[0].astype(jnp.float32) + near[1].astype(jnp.float32)
    for d in range(SEQ):
        blocks[d] = total[4 * d : 4 * d + 4].astype(jnp.bfloat16)

    def exchange(k, src, target):
        return pltpu.make_async_remote_copy(
            src_ref=blocks.at[target],
            dst_ref=landed.at[src],
            send_sem=a2a_send.at[k],
            recv_sem=a2a_recv.at[k],
            device_id=(target, y),
            device_id_type=MESH,
        )

    @pl.loop(1, SEQ)
    def _(k):
        exchange(k, me, lax.rem(me + k, SEQ)).start()

    own = pltpu.make_async_copy(blocks.at[me], landed.at[me], own_sem)
    own.start()
    own.wait()

    @pl.loop(1, SEQ)
    def _(k):
        exchange(k, lax.rem(me + SEQ - k, SEQ), lax.rem(me + k, SEQ)).wait_recv()

    for s in range(SEQ):
        arrived[4 * s : 4 * s + 4, :] = landed[s].astype(jnp.float32)

    @pl.loop(1, SEQ)
    def _(k):
        exchange(k, me, lax.rem(me + k, SEQ)).wait_send()

    for hop in hops:
        hop.wait_send()


def align(pooled, projector):
    vmem = pl.BlockSpec(memory_space=pltpu.VMEM)
    depth, width = projector.shape
    cols = width // 4
    return pl.pallas_call(
        align_kernel,
        out_shape=jax.ShapeDtypeStruct((SLOTS, cols), jnp.float32),
        in_specs=[vmem, pl.BlockSpec(memory_space=pl.ANY)],
        out_specs=vmem,
        scratch_shapes=[
            pltpu.VMEM((4, depth, cols), jnp.bfloat16),
            pltpu.VMEM((3, SLOTS, cols), jnp.bfloat16),
            pltpu.VMEM((2, SLOTS, cols), jnp.bfloat16),
            pltpu.VMEM((2, SLOTS // 2, cols), jnp.bfloat16),
            pltpu.VMEM((SEQ, 4, cols), jnp.bfloat16),
            pltpu.VMEM((SEQ, 4, cols), jnp.bfloat16),
            pltpu.SemaphoreType.DMA((4,)),
            pltpu.SemaphoreType.DMA((6,)),
            pltpu.SemaphoreType.DMA((6,)),
            pltpu.SemaphoreType.DMA((SEQ,)),
            pltpu.SemaphoreType.DMA((SEQ,)),
            pltpu.SemaphoreType.DMA,
        ],
        compiler_params=pltpu.CompilerParams(
            collective_id=1, has_side_effects=True, vmem_limit_bytes=VMEM_ALL
        ),
        name="align",
    )(pooled, projector)


def backward_kernel(
    sdocs, qback, gath, sctx, arrived, sspans, grad_q, terms,
    dstack, dq_t, own, blocks, own_sem, sem,
):
    window = Window(sdocs, gath, 2 * TG * HD, own, blocks, own_sem, sem, BB)
    window.start()
    width = SR * ROWS
    terms[...] = jnp.zeros(terms.shape, terms.dtype)
    member, weight, length = member_rows(sspans)
    columns = jnp.transpose(
        jnp.concatenate(
            [weight, (length > 0).astype(jnp.float32), jnp.zeros((6, SLOTS), jnp.float32)],
            axis=0,
        )
    )
    weight, live = columns[:, 0:1], columns[:, 1:2]
    member_t = jnp.transpose(member).astype(jnp.bfloat16)
    member = member.astype(jnp.bfloat16)
    pooled = dot(member_t, sctx[...]) * weight
    gap = jnp.where(live > 0.0, pooled - arrived[...], 0.0) * weight
    high = gap.astype(jnp.bfloat16)
    low = (gap - high.astype(jnp.float32)).astype(jnp.bfloat16)
    dout = (dot(member, high) + dot(member, low)).astype(jnp.bfloat16)
    lane = window.lanes[0]
    for h in range(SR):
        cols = slice(h * HD, (h + 1) * HD)
        head = dout[:, cols]
        delta = jnp.sum(
            head.astype(jnp.float32) * sctx[:, cols].astype(jnp.float32), axis=1, keepdims=True
        )
        marks = jnp.zeros((ROWS, 128), jnp.float32)
        for k, part in enumerate(parts(-delta)):
            marks = jnp.where(lane == ONES + k, part, marks)
        marks = marks.astype(jnp.bfloat16)
        top = slice(h * 128, (h + 1) * 128)
        rest = slice(SR * 128 + h * 32, SR * 128 + (h + 1) * 32)
        dstack[top, 0:HD] = head[0:128]
        dstack[rest, 0:HD] = head[128:160]
        dstack[top, HD:] = marks[0:128]
        dstack[rest, HD:] = marks[128:160]

    lanes_row = lane_rows(SR)

    def block(kv, marks, at, own_rows):
        count = kv.shape[0]
        rows = pl.ds(at, count)
        plain = kv[:, 0:HD]
        keys = jnp.concatenate([plain, marks], axis=1)
        values = jnp.concatenate([kv[:, HD:], marks], axis=1)
        keys_t = jnp.transpose(plain)
        grad_k = jnp.zeros((count, HD), jnp.float32)
        grad_v = jnp.zeros((count, HD), jnp.float32)
        for a, b in chunks(width):
            p = jnp.exp2(dot(keys, qback[a:b, :], NT) * EXP2_SCALE)
            if own_rows:
                p = jnp.where(own_pairs(a, b, lanes_row), p, 0.0)
            ds = (p * dot(values, dstack[a:b, :], NT)).astype(jnp.bfloat16)
            grad_v = grad_v + dot(p.astype(jnp.bfloat16), dstack[a:b, 0:HD])
            grad_k = grad_k + dot(ds, qback[a:b, 0:HD])
            add = dot(keys_t, ds)
            if own_rows:
                dq_t[:, a:b] = add
            else:
                dq_t[:, a:b] += add
        grad = jnp.concatenate([grad_k * SCALE, grad_v], axis=1)
        if not own_rows:
            grad = grad + terms[rows, :].astype(jnp.float32)
        terms[rows, :] = grad.astype(jnp.bfloat16)

    window.own_copy().wait()
    block(window.own, window.own_marks(), pl.multiple_of(window.place, 16), True)

    @pl.loop(0, window.steps)
    def _(step):
        window.copy(step).wait()
        block(window.blocks.at[step], window.marks(step), window.at(step), False)

    for h in range(SR):
        cols = slice(h * HD, (h + 1) * HD)
        grad_q[0:128, cols] = (jnp.transpose(dq_t[:, h * 128 : (h + 1) * 128]) * SCALE).astype(
            jnp.bfloat16
        )
    rest = (jnp.transpose(dq_t[:, SR * 128 :]) * SCALE).astype(jnp.bfloat16)
    for h in range(SR):
        grad_q[128:160, h * HD : (h + 1) * HD] = rest[h * 32 : (h + 1) * 32]


def backward(sdocs, qback, gath, sctx, arrived, sspans):
    vmem = pl.BlockSpec(memory_space=pltpu.VMEM)
    smem = pl.BlockSpec(memory_space=pltpu.SMEM)
    hbm = pl.BlockSpec(memory_space=pl.ANY)
    sw = SR * ROWS
    bf16 = jnp.bfloat16
    return pl.pallas_call(
        backward_kernel,
        out_shape=(
            jax.ShapeDtypeStruct((ROWS, SR * HD), bf16),
            jax.ShapeDtypeStruct((TOKENS, 2 * HD), bf16),
        ),
        in_specs=[smem, vmem, hbm, vmem, vmem, vmem],
        out_specs=(vmem, vmem),
        scratch_shapes=[
            pltpu.VMEM((sw, 2 * HD), bf16),
            pltpu.VMEM((HD, sw), jnp.float32),
            pltpu.VMEM((ROWS, 2 * HD), bf16),
            pltpu.VMEM((TOKENS // BB, BB, 2 * HD), bf16),
            pltpu.SemaphoreType.DMA,
            pltpu.SemaphoreType.DMA((TOKENS // BB,)),
        ],
        compiler_params=pltpu.CompilerParams(vmem_limit_bytes=VMEM_ALL),
        name="backward",
    )(sdocs, qback, gath, sctx, arrived, sspans)


def scatter_kernel(
    terms, grad_k, grad_v, theirs, chip, far1, near1, out1, far2, near2,
    die_send, die_recv, send_sem, recv_sem,
):
    me, z, x, c = place()
    y = lax.axis_index("mp")
    partner = seq_of(z, x, 1 - c)
    wrap = lambda v: lax.rem(v + 4, 4)

    def peer(axis, d):
        return seq_of(wrap(z + d), x, c) if axis == "z" else seq_of(z, wrap(x + d), c)

    greet(
        [(peer("z", 1), y), (peer("z", 3), y), (peer("x", 1), y), (peer("x", 3), y)]
        + [(partner, y)]
    )

    def crossing(i):
        return pltpu.make_async_remote_copy(
            src_ref=terms.at[pl.ds(4 * i, 4), 1 - c],
            dst_ref=theirs.at[pl.ds(4 * i, 4)],
            send_sem=die_send.at[i],
            recv_sem=die_recv.at[i],
            device_id=(partner, y),
            device_id_type=MESH,
        )

    for i in range(4):
        crossing(i).start()

    def remote(i, src, dst, target):
        return pltpu.make_async_remote_copy(
            src_ref=src,
            dst_ref=dst,
            send_sem=send_sem.at[i],
            recv_sem=recv_sem.at[i],
            device_id=(target, y),
            device_id_type=MESH,
        )

    for i in range(4):
        crossing(i).wait_recv()
        part = pl.ds(4 * i, 4)
        both = terms[part, c].astype(jnp.float32) + theirs[part].astype(jnp.float32)
        low = both.astype(jnp.bfloat16)
        chip[0, i] = low[:, 0:80]
        for j in range(4):
            chip[1, j, i] = low[j, 80:160]

    f32 = lambda v: v.astype(jnp.float32)
    all_hops = []
    axes = (("z", "x"), ("x", "z"))
    pos = ((z, x), (x, z))
    first = []
    for h in (0, 1):
        axis = axes[h][0]
        p = pos[h][0]
        up, down = peer(axis, 1), peer(axis, 3)
        to_far, to_up, to_down = wrap(p + 2), wrap(p + 1), wrap(p + 3)
        lo, hi = pl.ds(0, 2), pl.ds(2, 2)
        hops = [
            remote(12 * h + 0, chip.at[h, to_far, lo], far1.at[h, 0], up),
            remote(12 * h + 1, chip.at[h, to_far, hi], far1.at[h, 1], down),
            remote(12 * h + 2, chip.at[h, to_up, hi], near1.at[h, 0, hi], up),
            remote(12 * h + 3, chip.at[h, to_down, lo], near1.at[h, 1, lo], down),
            remote(12 * h + 4, chip.at[h, to_up, lo], near1.at[h, 0, lo], up),
            remote(12 * h + 5, chip.at[h, to_down, hi], near1.at[h, 1, hi], down),
        ]
        for k in range(4):
            hops[k].start()
        first.append((hops, to_up, to_down))
        all_hops += hops
    for h in (0, 1):
        hops, to_up, to_down = first[h]
        lo, hi = pl.ds(0, 2), pl.ds(2, 2)
        hops[0].wait_recv()
        chip[h, to_up, lo] = (f32(chip[h, to_up, lo]) + f32(far1[h, 0])).astype(jnp.bfloat16)
        hops[4].start()
        hops[1].wait_recv()
        chip[h, to_down, hi] = (f32(chip[h, to_down, hi]) + f32(far1[h, 1])).astype(jnp.bfloat16)
        hops[5].start()
    second = []
    for h in (0, 1):
        hops = first[h][0]
        for k in range(2, 6):
            hops[k].wait_recv()
        out1[h] = (f32(chip[h, pos[h][0]]) + f32(near1[h, 0]) + f32(near1[h, 1])).astype(
            jnp.bfloat16
        )
        axis = axes[h][1]
        p = pos[h][1]
        up, down = peer(axis, 1), peer(axis, 3)
        to_far, to_up, to_down = wrap(p + 2), wrap(p + 1), wrap(p + 3)
        lo, hi = pl.ds(0, HD), pl.ds(HD, HD)
        rows = pl.ds(0, 80)
        hops = [
            remote(12 * h + 6, out1.at[h, to_far, rows, lo], far2.at[h, 0], up),
            remote(12 * h + 7, out1.at[h, to_far, rows, hi], far2.at[h, 1], down),
            remote(12 * h + 8, out1.at[h, to_up, rows, hi], near2.at[h, 0, rows, hi], up),
            remote(12 * h + 9, out1.at[h, to_down, rows, lo], near2.at[h, 1, rows, lo], down),
            remote(12 * h + 10, out1.at[h, to_up, rows, lo], near2.at[h, 0, rows, lo], up),
            remote(12 * h + 11, out1.at[h, to_down, rows, hi], near2.at[h, 1, rows, hi], down),
        ]
        for k in range(4):
            hops[k].start()
        second.append((hops, to_up, to_down))
        all_hops += hops
    for h in (0, 1):
        hops, to_up, to_down = second[h]
        hops[0].wait_recv()
        out1[h, to_up, :, 0:HD] = (f32(out1[h, to_up, :, 0:HD]) + f32(far2[h, 0])).astype(
            jnp.bfloat16
        )
        hops[4].start()
        hops[1].wait_recv()
        out1[h, to_down, :, HD:] = (f32(out1[h, to_down, :, HD:]) + f32(far2[h, 1])).astype(
            jnp.bfloat16
        )
        hops[5].start()
    for h in (0, 1):
        hops = second[h][0]
        for k in range(2, 6):
            hops[k].wait_recv()
        total = (
            f32(out1[h, pos[h][1]]) + f32(near2[h, 0]) + f32(near2[h, 1])
        ).astype(jnp.bfloat16)
        grad_k[80 * h : 80 * h + 80, :] = total[:, 0:HD]
        grad_v[80 * h : 80 * h + 80, :] = total[:, HD:]
    for hop in all_hops:
        hop.wait_send()
    for i in range(4):
        crossing(i).wait_send()


def scatter(terms):
    vmem = pl.BlockSpec(memory_space=pltpu.VMEM)
    bf16 = jnp.bfloat16
    width = terms.shape[-1]
    return pl.pallas_call(
        scatter_kernel,
        out_shape=(
            jax.ShapeDtypeStruct((ROWS, HD), bf16),
            jax.ShapeDtypeStruct((ROWS, HD), bf16),
        ),
        in_specs=[vmem],
        out_specs=(vmem, vmem),
        scratch_shapes=[
            pltpu.VMEM((16, ROWS, width), bf16),
            pltpu.VMEM((2, 4, 4, 80, width), bf16),
            pltpu.VMEM((2, 2, 2, 80, width), bf16),
            pltpu.VMEM((2, 2, 4, 80, width), bf16),
            pltpu.VMEM((2, 4, 80, width), bf16),
            pltpu.VMEM((2, 2, 80, HD), bf16),
            pltpu.VMEM((2, 2, 80, width), bf16),
            pltpu.SemaphoreType.DMA((4,)),
            pltpu.SemaphoreType.DMA((4,)),
            pltpu.SemaphoreType.DMA((24,)),
            pltpu.SemaphoreType.DMA((24,)),
        ],
        compiler_params=pltpu.CompilerParams(
            collective_id=2, has_side_effects=True, vmem_limit_bytes=VMEM_ALL
        ),
        name="scatter",
    )(terms)


def body(
    teacher_query,
    teacher_keys,
    teacher_values,
    teacher_docs,
    student_query,
    student_keys,
    student_values,
    student_docs,
    projector,
    teacher_spans,
    student_spans,
):
    gath = gather(teacher_keys, teacher_values, student_keys, student_values)
    gath = gath.reshape(TOKENS, KV)
    pooled, sctx, qback = forward(
        teacher_docs, student_docs, teacher_query, student_query, gath, teacher_spans
    )
    arrived = align(pooled, projector)
    grad_q, terms = backward(student_docs, qback, gath, sctx, arrived, student_spans)
    grad_k, grad_v = scatter(terms.reshape(16, 2, ROWS, 2 * HD))
    return grad_q, grad_k, grad_v


def solution(mesh):
    return jax.shard_map(
        body,
        mesh=mesh,
        in_specs=(
            P("seq", "mp"),
            P("seq", "mp"),
            P("seq", "mp"),
            P(),
            P("seq", "mp"),
            P("seq", "mp"),
            P("seq", "mp"),
            P(),
            P("mp", None),
            P("seq", None, None),
            P("seq", None, None),
        ),
        out_specs=(P("seq", "mp"), P("seq", "mp"), P("seq", "mp")),
        check_vma=False,
    )
```

```python
import functools

import jax
import jax.numpy as jnp
from jax import lax
from jax.experimental import pallas as pl
from jax.experimental.pallas import tpu as pltpu
from jax.sharding import PartitionSpec as P

HD = 128
ROWS = 160
SEQ = 32
TOKENS = ROWS * SEQ
SLOTS = 128
TG, TR = 2, 8
SR = 7
MESH = pl.DeviceIdType.MESH
SCALE = HD**-0.5
EXP2_SCALE = SCALE * 1.4426950408889634
LOW = -1e30
MASKED = -3e38
NDOCS = 16
ONES, FLAG = NDOCS, NDOCS + 3
FAR = 1 << 20
FB = 512
BB = 512
SB = 640
TKV, SKV = 2 * TG * HD, 2 * HD
CHUNK = 1280
VMEM_ALL = 60 * 1024 * 1024

NT = (((1,), (1,)), ((), ()))
TN = (((0,), (0,)), ((), ()))


def dot(a, b, dims=None):
    if dims is None:
        dims = (((1,), (0,)), ((), ()))
    return lax.dot_general(a, b, dims, preferred_element_type=jnp.float32)


def place():
    me = lax.axis_index("seq")
    return me, me // 8, (me // 2) % 4, me % 2


def seq_of(z, x, c):
    return (z * 4 + x) * 2 + c


def greet(peers):
    barrier = pltpu.get_barrier_semaphore()
    for peer in peers:
        pl.semaphore_signal(barrier, inc=1, device_id=peer, device_id_type=MESH)
    pl.semaphore_wait(barrier, len(peers))


GATHER_OPS = 71


def seq_neighbours():
    me, z, x, c = place()
    wrap = lambda v: lax.rem(v + 4, 4)
    return [
        seq_of(z, wrap(x + 1), c),
        seq_of(z, wrap(x + 3), c),
        seq_of(wrap(z + 1), x, c),
        seq_of(wrap(z + 3), x, c),
        seq_of(z, x, 1 - c),
    ]


def torus_gather(buf, send_sem, recv_sem):
    me, z, x, c = place()
    y = lax.axis_index("mp")
    pos = ((x, z), (z, x))
    partner = seq_of(z, x, 1 - c)
    width = buf.shape[2]
    half_rows = ((0, ROWS // 2), (ROWS // 2, ROWS // 2))
    whole, left, right = (0, width), (0, width // 2), (width // 2, width // 2)
    ways = ((1, left), (-1, right))
    count = [0]
    started = []
    died = []

    def copy_of(i, slot, rows, cols, target):
        ref = buf.at[slot, pl.ds(*rows), pl.ds(*cols)]
        return pltpu.make_async_remote_copy(
            src_ref=ref,
            dst_ref=ref,
            send_sem=send_sem.at[i],
            recv_sem=recv_sem.at[i],
            device_id=(target, y),
            device_id_type=MESH,
        )

    def send(slot, rows, cols, target):
        i = count[0]
        count[0] += 1
        copy = copy_of(i, slot, rows, cols, target)
        copy.start()
        started.append(copy)
        return i

    def arrive(i, slot, rows, cols):
        copy_of(i, slot, rows, cols, partner).wait_recv()

    def both_cores(half, dp, dq):
        p, q = pos[half]
        zz, xx = (q + dq, p + dp) if half == 0 else (p + dp, q + dq)
        zz, xx = lax.rem(zz + 4, 4), lax.rem(xx + 4, 4)
        return seq_of(zz, xx, c), seq_of(zz, xx, 1 - c)

    def mine(half, dp, dq):
        return both_cores(half, dp, dq)[0]

    def die(slots, rows):
        slot, theirs = slots
        died.append((send(slot, rows, whole, partner), theirs, rows))

    first, second, across, further = {}, {}, {}, {}

    def spread(half, dp):
        rows = half_rows[half]
        for d in (1, -1):
            second[half, dp, d] = send(mine(half, dp, 0), rows, whole, mine(half, 0, d))
        die(both_cores(half, dp, 0), rows)

    def pass_on(half, dp):
        rows = half_rows[half]
        for d, cols in ways:
            slot = mine(half, dp, -d)
            arrive(second[half, dp, d], slot, rows, whole)
            further[half, dp, d] = send(slot, rows, cols, mine(half, 0, d))
            die(both_cores(half, dp, -d), rows)

    def ended(half, dp):
        rows = half_rows[half]
        for d, cols in ways:
            arrive(further[half, dp, d], mine(half, dp, -2 * d), rows, cols)
        die(both_cores(half, dp, 2), rows)

    for half in (0, 1):
        for d in (1, -1):
            first[half, d] = send(me, half_rows[half], whole, mine(half, d, 0))
    for half in (0, 1):
        for d in (1, -1):
            second[half, 0, d] = send(me, half_rows[half], whole, mine(half, 0, d))
    died.append((send(me, (0, ROWS), whole, partner), partner, (0, ROWS)))
    yield
    for d, cols in ways:
        for half in (0, 1):
            rows = half_rows[half]
            arrive(first[half, d], mine(half, -d, 0), rows, whole)
            across[half, d] = send(mine(half, -d, 0), rows, cols, mine(half, d, 0))
    for d in (1, -1):
        for half in (0, 1):
            spread(half, -d)
    yield
    for half in (0, 1):
        pass_on(half, 0)
    yield
    for half in (0, 1):
        for d, cols in ways:
            arrive(across[half, d], mine(half, -2 * d, 0), half_rows[half], cols)
        spread(half, 2)
    yield
    for dp in (-1, 1):
        for half in (0, 1):
            pass_on(half, dp)
    for half in (0, 1):
        ended(half, 0)
    yield
    for half in (0, 1):
        pass_on(half, 2)
    for dp in (-1, 1, 2):
        for half in (0, 1):
            ended(half, dp)
    for i, slot, rows in died:
        arrive(i, slot, rows, whole)
    yield
    for copy in started:
        copy.wait_send()
    assert count[0] == GATHER_OPS


def own_rows_in(refs, buf, sems):
    me = lax.axis_index("seq")
    copies = []
    at = 0
    for i, ref in enumerate(refs):
        width = ref.shape[1]
        copies.append(
            pltpu.make_async_copy(ref, buf.at[me, :, pl.ds(at, width)], sems.at[i])
        )
        at += width
    return copies


def doc_lanes(docs_ref):
    lane = lax.broadcasted_iota(jnp.int32, (1, 128), 1)
    first = jnp.where((lane >= ONES) & (lane < FLAG), -1, FAR)
    last = jnp.full((1, 128), FAR, jnp.int32)
    bound = jnp.int32(0)
    for k in range(NDOCS):
        first = jnp.where(lane == k, bound, first)
        bound = bound + docs_ref[k]
        last = jnp.where(lane == k, bound, last)
    return lane, first, last


def first_start(docs_ref, place_):
    bound = jnp.int32(0)
    lo = jnp.int32(0)
    for k in range(NDOCS):
        bound = bound + docs_ref[k]
        lo = jnp.where(bound <= place_, bound, lo)
    return lo


def key_marks(at, count, limit, lanes):
    lane, first, last = lanes
    first = jnp.where(lane == FLAG, limit, first)
    places = at + lax.broadcasted_iota(jnp.int32, (count, 128), 0)
    inside = (places >= first) & (places < last)
    return inside.astype(jnp.float32).astype(jnp.bfloat16)


def stack_heads(dst, src, first_head, ratio):
    for h in range(ratio):
        cols = slice((first_head + h) * HD, (first_head + h + 1) * HD)
        dst[h * 128 : (h + 1) * 128, 0:HD] = src[0:128, cols]
        dst[ratio * 128 + h * 32 : ratio * 128 + (h + 1) * 32, 0:HD] = src[128:160, cols]


def parts(value):
    high = value.astype(jnp.bfloat16).astype(jnp.float32)
    rest = value - high
    middle = rest.astype(jnp.bfloat16).astype(jnp.float32)
    return high, middle, rest - middle


def query_marks(places, shift, lanes):
    lane, first, last = lanes
    inside = (places >= first) & (places < last)
    marks = jnp.where((lane < NDOCS) & jnp.logical_not(inside) | (lane == FLAG), LOW, 0.0)
    for k, part in enumerate(parts(-shift)):
        marks = jnp.where(lane == ONES + k, part, marks)
    return marks.astype(jnp.bfloat16)


def mark_queries(dst, keys, place_, lanes, ratio):
    for begin, count, base in ((0, 128, 0), (128, 32, ratio * 128)):
        own = keys[begin : begin + count, :].astype(jnp.float32)
        places = place_ + begin + lax.broadcasted_iota(jnp.int32, (count, 1), 0)
        for h in range(ratio):
            rows = slice(base + h * count, base + (h + 1) * count)
            q = dst[rows, 0:HD].astype(jnp.float32)
            shift = jnp.sum(q * own, axis=1, keepdims=True)
            dst[rows, HD:] = query_marks(places, shift, lanes)


def lane_rows(ratio):
    lane = lax.broadcasted_iota(jnp.int32, (1, ratio * ROWS), 1)
    cut = ratio * 128
    return jnp.where(lane < cut, lane & 127, 128 + ((lane - cut) & 31))


def chunks(width):
    return [(a, min(a + CHUNK, width)) for a in range(0, width, CHUNK)]


def own_pairs(a, b, lanes_row):
    return lax.broadcasted_iota(jnp.int32, (ROWS, b - a), 0) <= lanes_row[:, a:b]


class Window:
    def __init__(self, docs_ref, gath, first_col, own, blocks, own_sem, sems, size):
        self.place = lax.axis_index("seq") * ROWS
        self.lo = first_start(docs_ref, self.place)
        self.size = size
        self.gath, self.own, self.blocks = gath, own, blocks
        self.own_sem, self.sems = own_sem, sems
        self.cols = pl.ds(first_col, own.shape[1])
        self.steps = (jnp.maximum(self.place - self.lo, 0) + size - 1) // size
        self.lanes = doc_lanes(docs_ref)

    def at(self, step):
        return pl.multiple_of(jnp.maximum(self.place - (step + 1) * self.size, 0), 16)

    def own_copy(self):
        rows = pl.ds(pl.multiple_of(self.place, 16), ROWS)
        return pltpu.make_async_copy(self.gath.at[rows, self.cols], self.own, self.own_sem)

    def copy(self, step):
        rows = pl.ds(self.at(step), self.size)
        return pltpu.make_async_copy(
            self.gath.at[rows, self.cols], self.blocks.at[step], self.sems.at[step]
        )

    def start(self):
        self.own_copy().start()

        @pl.loop(0, self.steps)
        def _(step):
            self.copy(step).start()

    def marks(self, step):
        return key_marks(
            self.at(step), self.size, self.place - step * self.size, self.lanes
        )

    def own_marks(self):
        return key_marks(self.place, ROWS, jnp.int32(FAR), self.lanes)


def extended(values):
    ones = jnp.ones((16, values.shape[0]), jnp.bfloat16)
    return jnp.concatenate([jnp.transpose(values), ones], axis=0)


class Attention:
    def __init__(self, queries, sums, acc, top, ratio):
        self.queries, self.sums, self.acc, self.top = queries, sums, acc, top
        self.lanes_row = lane_rows(ratio)
        self.chunks = chunks(ratio * ROWS)

    def pieces(self, kv, marks, own):
        groups = len(self.queries)
        for g in range(groups):
            keys = jnp.concatenate([kv[:, g * HD : (g + 1) * HD], marks], axis=1)
            values = extended(kv[:, (groups + g) * HD : (groups + g + 1) * HD])
            for a, b in self.chunks:
                s = dot(keys, self.queries[g][a:b, :], NT)
                if own:
                    s = jnp.where(own_pairs(a, b, self.lanes_row), s, MASKED)
                yield g, a, b, s, values

    def sum_rows(self, p):
        return jnp.sum(p.reshape(p.shape[0] // 8, 8, p.shape[1]), axis=0)

    def block(self, kv, marks, own):
        sums, acc = self.sums, self.acc
        if own:
            self.top[...] = jnp.zeros(self.top.shape, jnp.float32)
        for g, a, b, s, values in self.pieces(kv, marks, own):
            p = jnp.exp2(s * EXP2_SCALE)
            add = dot(values, p.astype(jnp.bfloat16))
            if sums is not None:
                total = self.sum_rows(p)
                sums[g, :, a:b] = total if own else sums[g, :, a:b] + total
            acc[g, :, a:b] = add if own else acc[g, :, a:b] + add

    def safe_block(self, kv, marks, own):
        sums, acc, top = self.sums, self.acc, self.top
        for g, a, b, s, values in self.pieces(kv, marks, own):
            old = jnp.full((1, b - a), LOW) if own else top[g, :, a:b]
            new = jnp.maximum(old, jnp.max(s, axis=0, keepdims=True))
            p = jnp.exp2((s - new) * EXP2_SCALE)
            add = dot(values, p.astype(jnp.bfloat16))
            top[g, :, a:b] = new
            alpha = None if own else jnp.exp2((old - new) * EXP2_SCALE)
            if sums is not None:
                total = self.sum_rows(p)
                sums[g, :, a:b] = total if own else sums[g, :, a:b] * alpha + total
            acc[g, :, a:b] = add if own else acc[g, :, a:b] * alpha + add

    def safe_window(self, window):
        self.safe_block(window.own, window.own_marks(), True)

        @pl.loop(0, window.steps)
        def _(step):
            self.safe_block(window.blocks.at[step], window.marks(step), False)


def too_large(weight_sums):
    return jnp.logical_not(jnp.max(weight_sums) < 2.0**100)


def member_rows(spans_ref):
    start = spans_ref[0, 0:1, :]
    length = spans_ref[0, 1:2, :]
    row = lax.broadcasted_iota(jnp.int32, (ROWS, SLOTS), 0)
    inside = (row >= start) & (row < start + length)
    weight = 1.0 / jnp.maximum(length, 1).astype(jnp.float32)
    return inside.astype(jnp.float32), weight, length


def forward_kernel(
    tdocs, tq, gath, tspans, pooled, stack, own, blocks, acc, top, own_sem, sem
):
    window = Window(tdocs, gath, 0, own, blocks, own_sem, sem, FB)
    window.start()
    for g in range(TG):
        stack_heads(stack.at[g], tq, g * TR, TR)
    window.own_copy().wait()
    for g in range(TG):
        mark_queries(
            stack.at[g], own.at[:, g * HD : (g + 1) * HD], window.place, window.lanes, TR
        )
    attention = Attention([stack.at[g] for g in range(TG)], None, acc, top, TR)
    attention.block(own, window.own_marks(), True)

    @pl.loop(0, window.steps)
    def _(step):
        window.copy(step).wait()
        attention.block(blocks.at[step], window.marks(step), False)

    @pl.when(too_large(acc[:, HD : HD + 8, :]))
    def _():
        attention.safe_window(window)

    member, weight, _ = member_rows(tspans)
    member = member.astype(jnp.bfloat16)
    tail = jnp.concatenate([member[128:160]] * TR, axis=0)
    owner = lax.broadcasted_iota(jnp.int32, (TR * 32, SLOTS), 0) // 32
    for g in range(TG):
        inverse = 1.0 / acc[g, HD : HD + 1]
        context_t = (acc[g, 0:HD] * inverse).astype(jnp.bfloat16)
        for h in range(TR):
            sums = dot(context_t[:, h * 128 : (h + 1) * 128], member[0:128]) + dot(
                context_t[:, TR * 128 :], jnp.where(owner == h, tail, jnp.zeros_like(tail))
            )
            cols = slice((g * TR + h) * HD, (g * TR + h + 1) * HD)
            pooled[:, cols] = jnp.transpose(sums * weight).astype(jnp.bfloat16)


def forward(tdocs, tq, gath, tspans):
    vmem = pl.BlockSpec(memory_space=pltpu.VMEM)
    smem = pl.BlockSpec(memory_space=pltpu.SMEM)
    hbm = pl.BlockSpec(memory_space=pl.ANY)
    tw = TR * ROWS
    bf16, f32 = jnp.bfloat16, jnp.float32
    return pl.pallas_call(
        forward_kernel,
        out_shape=jax.ShapeDtypeStruct((SLOTS, TG * TR * HD), bf16),
        in_specs=[smem, vmem, hbm, vmem],
        out_specs=vmem,
        scratch_shapes=[
            pltpu.VMEM((TG, tw, 2 * HD), bf16),
            pltpu.VMEM((ROWS, 2 * TG * HD), bf16),
            pltpu.VMEM((TOKENS // FB, FB, 2 * TG * HD), bf16),
            pltpu.VMEM((TG, HD + 16, tw), f32),
            pltpu.VMEM((TG, 1, tw), f32),
            pltpu.SemaphoreType.DMA,
            pltpu.SemaphoreType.DMA((TOKENS // FB,)),
        ],
        compiler_params=pltpu.CompilerParams(vmem_limit_bytes=VMEM_ALL),
        name="forward",
    )(tdocs, tq, gath, tspans)


def student_results(attention, stack, lanes, sctx, qback):
    acc = attention.acc
    total = jnp.sum(attention.sums[0], axis=0, keepdims=True)
    inverse = 1.0 / acc[0, HD : HD + 1]
    extra = attention.top[0] + jnp.log2(total) * (1.0 / EXP2_SCALE)
    for h in range(SR):
        cols = slice(h * 128, (h + 1) * 128)
        sctx[0:128, cols] = jnp.transpose(acc[0, 0:HD, cols] * inverse[:, cols]).astype(
            jnp.bfloat16
        )
    rest = jnp.transpose(acc[0, 0:HD, SR * 128 :] * inverse[:, SR * 128 :]).astype(jnp.bfloat16)
    for h in range(SR):
        sctx[128:160, h * HD : (h + 1) * HD] = rest[h * 32 : (h + 1) * 32]
    qback[:, 0:HD] = stack[:, 0:HD]
    lane = lanes[0]
    ones = (lane >= ONES) & (lane < FLAG)
    for a in range(0, SR * ROWS, 128):
        b = min(a + 128, SR * ROWS)
        column = jnp.transpose(jnp.broadcast_to(extra[:, a:b], (8, b - a)))[:, 0:1]
        marks = stack[a:b, HD:].astype(jnp.float32)
        before = jnp.sum(jnp.where(ones, marks, 0.0), axis=1, keepdims=True)
        for k, part in enumerate(parts(before - column)):
            marks = jnp.where(lane == ONES + k, part, marks)
        qback[a:b, HD:] = marks.astype(jnp.bfloat16)


def gather_kernel(tk, tv, sk, sv, gath, own_sem, send_sem, recv_sem):
    y = lax.axis_index("mp")
    copies = own_rows_in((tk, tv, sk, sv), gath, own_sem)
    for copy in copies:
        copy.start()
    greet([(peer, y) for peer in seq_neighbours()])
    for copy in copies:
        copy.wait()
    for _ in torus_gather(gath, send_sem, recv_sem):
        pass


def gather(tk, tv, sk, sv):
    hbm = pl.BlockSpec(memory_space=pl.ANY)
    return pl.pallas_call(
        gather_kernel,
        out_shape=jax.ShapeDtypeStruct((SEQ, ROWS, TKV + SKV), jnp.bfloat16),
        in_specs=[hbm] * 4,
        out_specs=pl.BlockSpec(memory_space=pltpu.VMEM),
        scratch_shapes=[
            pltpu.SemaphoreType.DMA((4,)),
            pltpu.SemaphoreType.DMA((GATHER_OPS,)),
            pltpu.SemaphoreType.DMA((GATHER_OPS,)),
        ],
        compiler_params=pltpu.CompilerParams(
            collective_id=0, has_side_effects=True, vmem_limit_bytes=VMEM_ALL
        ),
        name="gather",
    )(tk, tv, sk, sv)


def align_kernel(
    sdocs, pooled, projector, gath, sk, sv, sq, arrived, sctx, qback, weight_sums,
    wide, part, near, far, blocks, landed, kv, stack, sums, acc, top,
    load_sem, send_sem, recv_sem, a2a_send, a2a_recv, own_sem,
):
    me = lax.axis_index("seq")
    y = lax.axis_index("mp")
    cols = part.shape[2]
    half = SLOTS // 2
    up, down, across = lax.rem(y + 1, 4), lax.rem(y + 3, 4), lax.rem(y + 2, 4)
    order = (across, up, down, y)
    loads = []
    for i, target in enumerate(order):
        begin = pl.multiple_of(target * cols, 128)
        copy = pltpu.make_async_copy(
            projector.at[:, pl.ds(begin, cols)], wide.at[i], load_sem.at[i]
        )
        copy.start()
        loads.append(copy)
    student = pltpu.make_async_copy(gath.at[:, pl.ds(TKV, SKV)], kv, own_sem.at[1])
    student.start()

    barrier = pltpu.get_barrier_semaphore()
    for target in (up, down):
        pl.semaphore_signal(barrier, inc=1, device_id=(me, target), device_id_type=MESH)

    @pl.loop(1, SEQ)
    def _(k):
        pl.semaphore_signal(
            barrier, inc=1, device_id=(lax.rem(me + k, SEQ), y), device_id_type=MESH
        )

    pl.semaphore_wait(barrier, SEQ + 1)

    def project(i):
        loads[i].wait()
        return dot(pooled[...], wide[i])

    def remote(i, src, dst, target):
        return pltpu.make_async_remote_copy(
            src_ref=src,
            dst_ref=dst,
            send_sem=send_sem.at[i],
            recv_sem=recv_sem.at[i],
            device_id=(me, target),
            device_id_type=MESH,
        )

    low, high = pl.ds(0, half), pl.ds(half, half)
    hops = [
        remote(0, part.at[0, low], far.at[0], up),
        remote(1, part.at[0, high], far.at[1], down),
        remote(2, part.at[1, high], near.at[0, high], up),
        remote(3, part.at[2, low], near.at[1, low], down),
        remote(4, part.at[1, low], near.at[0, low], up),
        remote(5, part.at[2, high], near.at[1, high], down),
    ]
    part[0] = project(0).astype(jnp.bfloat16)
    hops[0].start()
    hops[1].start()
    for_up = project(1)
    part[1, half:] = for_up[half:].astype(jnp.bfloat16)
    hops[2].start()
    for_down = project(2)
    part[2, :half] = for_down[:half].astype(jnp.bfloat16)
    hops[3].start()
    place_ = me * ROWS
    lanes = doc_lanes(sdocs)
    stack_heads(stack, sq, 0, SR)
    mark_queries(stack, sk[...], place_, lanes, SR)
    attention = Attention([stack], sums, acc, top, SR)
    attention.block(
        jnp.concatenate([sk[...], sv[...]], axis=1),
        key_marks(place_, ROWS, jnp.int32(FAR), lanes),
        True,
    )
    count = (place_ + SB - 1) // SB

    def student_blocks(first, last):
        @pl.loop(first, last)
        def _(b):
            rows = pl.ds(pl.multiple_of(b * SB, SB), SB)
            attention.block(kv[rows], key_marks(b * SB, SB, place_, lanes), False)

    student.wait()
    hops[0].wait_recv()
    part[1, :half] = (for_up[:half] + far[0].astype(jnp.float32)).astype(jnp.bfloat16)
    hops[4].start()
    hops[1].wait_recv()
    part[2, half:] = (for_down[half:] + far[1].astype(jnp.float32)).astype(jnp.bfloat16)
    hops[5].start()
    mine = project(3)
    student_blocks(0, count // 2)
    for i in (2, 3, 4, 5):
        hops[i].wait_recv()
    total = mine + near[0].astype(jnp.float32) + near[1].astype(jnp.float32)
    for d in range(SEQ):
        blocks[d] = total[4 * d : 4 * d + 4].astype(jnp.bfloat16)

    def exchange(k, src, target):
        return pltpu.make_async_remote_copy(
            src_ref=blocks.at[target],
            dst_ref=landed.at[src],
            send_sem=a2a_send.at[k],
            recv_sem=a2a_recv.at[k],
            device_id=(target, y),
            device_id_type=MESH,
        )

    @pl.loop(1, SEQ)
    def _(k):
        exchange(k, me, lax.rem(me + k, SEQ)).start()

    own = pltpu.make_async_copy(blocks.at[me], landed.at[me], own_sem.at[0])
    own.start()
    student_blocks(count // 2, count)
    weight_sums[...] = acc[0, HD : HD + 8, :]
    student_results(attention, stack, lanes, sctx, qback)
    own.wait()

    @pl.loop(1, SEQ)
    def _(k):
        exchange(k, lax.rem(me + SEQ - k, SEQ), lax.rem(me + k, SEQ)).wait_recv()

    for s in range(SEQ):
        arrived[4 * s : 4 * s + 4, :] = landed[s].astype(jnp.float32)

    @pl.loop(1, SEQ)
    def _(k):
        exchange(k, me, lax.rem(me + k, SEQ)).wait_send()

    for hop in hops:
        hop.wait_send()


def align(sdocs, pooled, projector, gath, sk, sv, sq):
    vmem = pl.BlockSpec(memory_space=pltpu.VMEM)
    smem = pl.BlockSpec(memory_space=pltpu.SMEM)
    hbm = pl.BlockSpec(memory_space=pl.ANY)
    depth, width = projector.shape
    cols = width // 4
    sw = SR * ROWS
    bf16, f32 = jnp.bfloat16, jnp.float32
    return pl.pallas_call(
        align_kernel,
        out_shape=(
            jax.ShapeDtypeStruct((SLOTS, cols), f32),
            jax.ShapeDtypeStruct((ROWS, SR * HD), bf16),
            jax.ShapeDtypeStruct((sw, 2 * HD), bf16),
            jax.ShapeDtypeStruct((8, sw), f32),
        ),
        in_specs=[smem, vmem, hbm, hbm, vmem, vmem, vmem],
        out_specs=(vmem,) * 4,
        scratch_shapes=[
            pltpu.VMEM((4, depth, cols), bf16),
            pltpu.VMEM((3, SLOTS, cols), bf16),
            pltpu.VMEM((2, SLOTS, cols), bf16),
            pltpu.VMEM((2, SLOTS // 2, cols), bf16),
            pltpu.VMEM((SEQ, 4, cols), bf16),
            pltpu.VMEM((SEQ, 4, cols), bf16),
            pltpu.VMEM((TOKENS, SKV), bf16),
            pltpu.VMEM((sw, 2 * HD), bf16),
            pltpu.VMEM((1, 8, sw), f32),
            pltpu.VMEM((1, HD + 16, sw), f32),
            pltpu.VMEM((1, 1, sw), f32),
            pltpu.SemaphoreType.DMA((4,)),
            pltpu.SemaphoreType.DMA((6,)),
            pltpu.SemaphoreType.DMA((6,)),
            pltpu.SemaphoreType.DMA((SEQ,)),
            pltpu.SemaphoreType.DMA((SEQ,)),
            pltpu.SemaphoreType.DMA((2,)),
        ],
        compiler_params=pltpu.CompilerParams(
            collective_id=1, has_side_effects=True, vmem_limit_bytes=VMEM_ALL
        ),
        name="align",
    )(sdocs, pooled, projector, gath, sk, sv, sq)


def backward_kernel(
    sdocs, qback_in, gath, sctx_in, weight_sums, sq, arrived, sspans, grad_q, terms,
    dstack, dq_t, own, blocks, qback, sctx, stack, sums, acc, top, own_sem, sem,
):
    window = Window(sdocs, gath, TKV, own, blocks, own_sem, sem, BB)
    window.start()
    qback[...] = qback_in[...]
    sctx[...] = sctx_in[...]
    window.own_copy().wait()

    @pl.loop(0, window.steps)
    def _(step):
        window.copy(step).wait()

    @pl.when(too_large(weight_sums[...]))
    def _():
        stack_heads(stack, sq, 0, SR)
        mark_queries(stack, own.at[:, 0:HD], window.place, window.lanes, SR)
        attention = Attention([stack], sums, acc, top, SR)
        attention.safe_window(window)
        student_results(attention, stack, window.lanes, sctx, qback)

    width = SR * ROWS
    terms[...] = jnp.zeros(terms.shape, terms.dtype)
    member, weight, length = member_rows(sspans)
    columns = jnp.transpose(
        jnp.concatenate(
            [weight, (length > 0).astype(jnp.float32), jnp.zeros((6, SLOTS), jnp.float32)],
            axis=0,
        )
    )
    weight, live = columns[:, 0:1], columns[:, 1:2]
    member_t = jnp.transpose(member).astype(jnp.bfloat16)
    member = member.astype(jnp.bfloat16)
    pooled = dot(member_t, sctx[...]) * weight
    gap = jnp.where(live > 0.0, pooled - arrived[...], 0.0) * weight
    high = gap.astype(jnp.bfloat16)
    low = (gap - high.astype(jnp.float32)).astype(jnp.bfloat16)
    dout = (dot(member, high) + dot(member, low)).astype(jnp.bfloat16)
    lane = window.lanes[0]
    for h in range(SR):
        cols = slice(h * HD, (h + 1) * HD)
        head = dout[:, cols]
        delta = jnp.sum(
            head.astype(jnp.float32) * sctx[:, cols].astype(jnp.float32), axis=1, keepdims=True
        )
        marks = jnp.zeros((ROWS, 128), jnp.float32)
        for k, part in enumerate(parts(-delta)):
            marks = jnp.where(lane == ONES + k, part, marks)
        marks = marks.astype(jnp.bfloat16)
        top = slice(h * 128, (h + 1) * 128)
        rest = slice(SR * 128 + h * 32, SR * 128 + (h + 1) * 32)
        dstack[top, 0:HD] = head[0:128]
        dstack[rest, 0:HD] = head[128:160]
        dstack[top, HD:] = marks[0:128]
        dstack[rest, HD:] = marks[128:160]

    lanes_row = lane_rows(SR)

    def block(kv, marks, at, own_rows):
        count = kv.shape[0]
        rows = pl.ds(at, count)
        plain = kv[:, 0:HD]
        keys = jnp.concatenate([plain, marks], axis=1)
        values = jnp.concatenate([kv[:, HD:], marks], axis=1)
        keys_t = jnp.transpose(plain)
        grad_k = jnp.zeros((count, HD), jnp.float32)
        grad_v = jnp.zeros((count, HD), jnp.float32)
        for a, b in chunks(width):
            p = jnp.exp2(dot(keys, qback[a:b, :], NT) * EXP2_SCALE)
            if own_rows:
                p = jnp.where(own_pairs(a, b, lanes_row), p, 0.0)
            ds = (p * dot(values, dstack[a:b, :], NT)).astype(jnp.bfloat16)
            grad_v = grad_v + dot(p.astype(jnp.bfloat16), dstack[a:b, 0:HD])
            grad_k = grad_k + dot(ds, qback[a:b, 0:HD])
            add = dot(keys_t, ds)
            if own_rows:
                dq_t[:, a:b] = add
            else:
                dq_t[:, a:b] += add
        grad = jnp.concatenate([grad_k * SCALE, grad_v], axis=1)
        if not own_rows:
            grad = grad + terms[rows, :].astype(jnp.float32)
        terms[rows, :] = grad.astype(jnp.bfloat16)

    block(window.own, window.own_marks(), pl.multiple_of(window.place, 16), True)

    @pl.loop(0, window.steps)
    def _(step):
        block(window.blocks.at[step], window.marks(step), window.at(step), False)

    for h in range(SR):
        cols = slice(h * HD, (h + 1) * HD)
        grad_q[0:128, cols] = (jnp.transpose(dq_t[:, h * 128 : (h + 1) * 128]) * SCALE).astype(
            jnp.bfloat16
        )
    rest = (jnp.transpose(dq_t[:, SR * 128 :]) * SCALE).astype(jnp.bfloat16)
    for h in range(SR):
        grad_q[128:160, h * HD : (h + 1) * HD] = rest[h * 32 : (h + 1) * 32]


def backward(sdocs, qback, gath, sctx, weight_sums, sq, arrived, sspans):
    vmem = pl.BlockSpec(memory_space=pltpu.VMEM)
    smem = pl.BlockSpec(memory_space=pltpu.SMEM)
    hbm = pl.BlockSpec(memory_space=pl.ANY)
    sw = SR * ROWS
    bf16 = jnp.bfloat16
    return pl.pallas_call(
        backward_kernel,
        out_shape=(
            jax.ShapeDtypeStruct((ROWS, SR * HD), bf16),
            jax.ShapeDtypeStruct((TOKENS, 2 * HD), bf16),
        ),
        in_specs=[smem, vmem, hbm, vmem, vmem, vmem, vmem, vmem],
        out_specs=(vmem, vmem),
        scratch_shapes=[
            pltpu.VMEM((sw, 2 * HD), bf16),
            pltpu.VMEM((HD, sw), jnp.float32),
            pltpu.VMEM((ROWS, 2 * HD), bf16),
            pltpu.VMEM((TOKENS // BB, BB, 2 * HD), bf16),
            pltpu.VMEM((sw, 2 * HD), bf16),
            pltpu.VMEM((ROWS, SR * HD), bf16),
            pltpu.VMEM((sw, 2 * HD), bf16),
            pltpu.VMEM((1, 8, sw), jnp.float32),
            pltpu.VMEM((1, HD + 16, sw), jnp.float32),
            pltpu.VMEM((1, 1, sw), jnp.float32),
            pltpu.SemaphoreType.DMA,
            pltpu.SemaphoreType.DMA((TOKENS // BB,)),
        ],
        compiler_params=pltpu.CompilerParams(vmem_limit_bytes=VMEM_ALL),
        name="backward",
    )(sdocs, qback, gath, sctx, weight_sums, sq, arrived, sspans)


def scatter_kernel(
    terms, pieces, theirs, chip, far1, near1, out1, far2,
    die_send, die_recv, send_sem, recv_sem,
):
    me, z, x, c = place()
    y = lax.axis_index("mp")
    partner = seq_of(z, x, 1 - c)
    wrap = lambda v: lax.rem(v + 4, 4)

    def peer(axis, d):
        return seq_of(wrap(z + d), x, c) if axis == "z" else seq_of(z, wrap(x + d), c)

    greet(
        [(peer("z", 1), y), (peer("z", 3), y), (peer("x", 1), y), (peer("x", 3), y)]
        + [(partner, y)]
    )

    f32 = lambda v: v.astype(jnp.float32)
    axes = (("z", "x"), ("x", "z"))
    pos = ((z, x), (x, z))

    def terms_of(h, i, core):
        rows = pl.ds(80 * h, 80)
        return terms.at[i, :, core, rows] if h == 0 else terms.at[:, i, core, rows]

    order = (2, 1, 3, 0)

    def crossing(h, k):
        i = wrap(pos[h][0] + order[k])
        return pltpu.make_async_remote_copy(
            src_ref=terms_of(h, i, 1 - c),
            dst_ref=theirs.at[h, i],
            send_sem=die_send.at[4 * h + k],
            recv_sem=die_recv.at[4 * h + k],
            device_id=(partner, y),
            device_id_type=MESH,
        )

    def both_cores(h, k):
        i = wrap(pos[h][0] + order[k])
        crossing(h, k).wait_recv()
        chip[h, i] = (f32(terms_of(h, i, c)[...]) + f32(theirs[h, i])).astype(jnp.bfloat16)

    for k in range(4):
        for h in (0, 1):
            crossing(h, k).start()

    def remote(i, src, dst, target):
        return pltpu.make_async_remote_copy(
            src_ref=src,
            dst_ref=dst,
            send_sem=send_sem.at[i],
            recv_sem=recv_sem.at[i],
            device_id=(target, y),
            device_id_type=MESH,
        )

    all_hops = []
    first = []
    for h in (0, 1):
        axis = axes[h][0]
        p = pos[h][0]
        up, down = peer(axis, 1), peer(axis, 3)
        to_far, to_up, to_down = wrap(p + 2), wrap(p + 1), wrap(p + 3)
        lo, hi = pl.ds(0, 2), pl.ds(2, 2)
        hops = [
            remote(12 * h + 0, chip.at[h, to_far, lo], far1.at[h, 0], up),
            remote(12 * h + 1, chip.at[h, to_far, hi], far1.at[h, 1], down),
            remote(12 * h + 2, chip.at[h, to_up, hi], near1.at[h, 0, hi], up),
            remote(12 * h + 3, chip.at[h, to_down, lo], near1.at[h, 1, lo], down),
            remote(12 * h + 4, chip.at[h, to_up, lo], near1.at[h, 0, lo], up),
            remote(12 * h + 5, chip.at[h, to_down, hi], near1.at[h, 1, hi], down),
        ]
        first.append((hops, to_up, to_down))
        all_hops += hops
    for k, ready in enumerate(((0, 1), (2,), (3,), ())):
        for h in (0, 1):
            both_cores(h, k)
            for i in ready:
                first[h][0][i].start()
    for h in (0, 1):
        hops, to_up, to_down = first[h]
        lo, hi = pl.ds(0, 2), pl.ds(2, 2)
        hops[0].wait_recv()
        chip[h, to_up, lo] = (f32(chip[h, to_up, lo]) + f32(far1[h, 0])).astype(jnp.bfloat16)
        hops[4].start()
        hops[1].wait_recv()
        chip[h, to_down, hi] = (f32(chip[h, to_down, hi]) + f32(far1[h, 1])).astype(jnp.bfloat16)
        hops[5].start()
    second = []
    for h in (0, 1):
        hops = first[h][0]
        for k in range(2, 6):
            hops[k].wait_recv()
        out1[h] = (f32(chip[h, pos[h][0]]) + f32(near1[h, 0]) + f32(near1[h, 1])).astype(
            jnp.bfloat16
        )
        axis = axes[h][1]
        p = pos[h][1]
        up, down = peer(axis, 1), peer(axis, 3)
        to_far, to_up, to_down = wrap(p + 2), wrap(p + 1), wrap(p + 3)
        lo, hi = pl.ds(0, HD), pl.ds(HD, HD)
        rows = pl.ds(0, 80)
        hops = [
            remote(12 * h + 6, out1.at[h, to_far, rows, lo], far2.at[h, 0], up),
            remote(12 * h + 7, out1.at[h, to_far, rows, hi], far2.at[h, 1], down),
            remote(12 * h + 8, out1.at[h, to_up, rows, hi], pieces.at[h, 1, rows, hi], up),
            remote(12 * h + 9, out1.at[h, to_down, rows, lo], pieces.at[h, 2, rows, lo], down),
            remote(12 * h + 10, out1.at[h, to_up, rows, lo], pieces.at[h, 1, rows, lo], up),
            remote(12 * h + 11, out1.at[h, to_down, rows, hi], pieces.at[h, 2, rows, hi], down),
        ]
        for k in range(4):
            hops[k].start()
        second.append((hops, to_up, to_down))
        all_hops += hops
    for h in (0, 1):
        hops, to_up, to_down = second[h]
        hops[0].wait_recv()
        out1[h, to_up, :, 0:HD] = (f32(out1[h, to_up, :, 0:HD]) + f32(far2[h, 0])).astype(
            jnp.bfloat16
        )
        hops[4].start()
        hops[1].wait_recv()
        out1[h, to_down, :, HD:] = (f32(out1[h, to_down, :, HD:]) + f32(far2[h, 1])).astype(
            jnp.bfloat16
        )
        hops[5].start()
    for h in (0, 1):
        hops = second[h][0]
        for k in range(2, 6):
            hops[k].wait_recv()
        pieces[h, 0] = out1[h, pos[h][1]]
    for hop in all_hops:
        hop.wait_send()
    for h in (0, 1):
        for k in range(4):
            crossing(h, k).wait_send()


def scatter(terms):
    vmem = pl.BlockSpec(memory_space=pltpu.VMEM)
    bf16 = jnp.bfloat16
    width = terms.shape[-1]
    return pl.pallas_call(
        scatter_kernel,
        out_shape=jax.ShapeDtypeStruct((2, 3, 80, width), bf16),
        in_specs=[vmem],
        out_specs=vmem,
        scratch_shapes=[
            pltpu.VMEM((2, 4, 4, 80, width), bf16),
            pltpu.VMEM((2, 4, 4, 80, width), bf16),
            pltpu.VMEM((2, 2, 2, 80, width), bf16),
            pltpu.VMEM((2, 2, 4, 80, width), bf16),
            pltpu.VMEM((2, 4, 80, width), bf16),
            pltpu.VMEM((2, 2, 80, HD), bf16),
            pltpu.SemaphoreType.DMA((8,)),
            pltpu.SemaphoreType.DMA((8,)),
            pltpu.SemaphoreType.DMA((24,)),
            pltpu.SemaphoreType.DMA((24,)),
        ],
        compiler_params=pltpu.CompilerParams(
            collective_id=2, has_side_effects=True, vmem_limit_bytes=VMEM_ALL
        ),
        name="scatter",
    )(terms)


def total_kernel(pieces, grad_k, grad_v):
    for h in (0, 1):
        rows = slice(80 * h, 80 * h + 80)
        total = sum(pieces[h, k].astype(jnp.float32) for k in range(3)).astype(jnp.bfloat16)
        grad_k[rows, :] = total[:, 0:HD]
        grad_v[rows, :] = total[:, HD:]


def total(pieces):
    vmem = pl.BlockSpec(memory_space=pltpu.VMEM)
    return pl.pallas_call(
        total_kernel,
        out_shape=(jax.ShapeDtypeStruct((ROWS, HD), jnp.bfloat16),) * 2,
        in_specs=[vmem],
        out_specs=(vmem, vmem),
        name="total",
    )(pieces)


def body(
    teacher_query,
    teacher_keys,
    teacher_values,
    teacher_docs,
    student_query,
    student_keys,
    student_values,
    student_docs,
    projector,
    teacher_spans,
    student_spans,
):
    gath = gather(teacher_keys, teacher_values, student_keys, student_values)
    gath = gath.reshape(TOKENS, TKV + SKV)
    pooled = forward(teacher_docs, teacher_query, gath, teacher_spans)
    arrived, sctx, qback, weight_sums = align(
        student_docs, pooled, projector, gath, student_keys, student_values, student_query
    )
    grad_q, terms = backward(
        student_docs, qback, gath, sctx, weight_sums, student_query, arrived, student_spans
    )
    grad_k, grad_v = total(scatter(terms.reshape(4, 4, 2, ROWS, 2 * HD)))
    return grad_q, grad_k, grad_v


def solution(mesh):
    return jax.shard_map(
        body,
        mesh=mesh,
        in_specs=(
            P("seq", "mp"),
            P("seq", "mp"),
            P("seq", "mp"),
            P(),
            P("seq", "mp"),
            P("seq", "mp"),
            P("seq", "mp"),
            P(),
            P("mp", None),
            P("seq", None, None),
            P("seq", None, None),
        ),
        out_specs=(P("seq", "mp"), P("seq", "mp"), P("seq", "mp")),
        check_vma=False,
    )
```

```python
import functools

import jax
import jax.numpy as jnp
from jax import lax
from jax.experimental import pallas as pl
from jax.experimental.pallas import tpu as pltpu
from jax.sharding import PartitionSpec as P

HD = 128
ROWS = 160
SEQ = 32
TOKENS = ROWS * SEQ
SLOTS = 128
TG, TR = 2, 8
SR = 7
MESH = pl.DeviceIdType.MESH
SCALE = HD**-0.5
EXP2_SCALE = SCALE * 1.4426950408889634
LOW = -1e30
MASKED = -3e38
NDOCS = 16
ONES, FLAG = NDOCS, NDOCS + 3
FAR = 1 << 20
FB = 768
BB = 768
SB = 640
STEPS = -(-TOKENS // FB)
TKV, SKV = 2 * TG * HD, 2 * HD
CHUNK = 1280
MIB = 1 << 20

NT = (((1,), (1,)), ((), ()))
TN = (((0,), (0,)), ((), ()))


def dot(a, b, dims=None):
    if dims is None:
        dims = (((1,), (0,)), ((), ()))
    return lax.dot_general(a, b, dims, preferred_element_type=jnp.float32)


def place():
    me = lax.axis_index("seq")
    return me, me // 8, (me // 2) % 4, me % 2


def seq_of(z, x, c):
    return (z * 4 + x) * 2 + c


def greet(peers):
    barrier = pltpu.get_barrier_semaphore()
    for peer in peers:
        pl.semaphore_signal(barrier, inc=1, device_id=peer, device_id_type=MESH)
    pl.semaphore_wait(barrier, len(peers))


GATHER_OPS = 71


def seq_neighbours():
    me, z, x, c = place()
    wrap = lambda v: lax.rem(v + 4, 4)
    return [
        seq_of(z, wrap(x + 1), c),
        seq_of(z, wrap(x + 3), c),
        seq_of(wrap(z + 1), x, c),
        seq_of(wrap(z + 3), x, c),
        seq_of(z, x, 1 - c),
    ]


def torus_gather(buf, send_sem, recv_sem):
    me, z, x, c = place()
    y = lax.axis_index("mp")
    pos = ((x, z), (z, x))
    partner = seq_of(z, x, 1 - c)
    width = buf.shape[2]
    half_rows = ((0, ROWS // 2), (ROWS // 2, ROWS // 2))
    whole, left, right = (0, width), (0, width // 2), (width // 2, width // 2)
    ways = ((1, left), (-1, right))
    count = [0]
    started = []
    died = []

    def copy_of(i, slot, rows, cols, target):
        ref = buf.at[slot, pl.ds(*rows), pl.ds(*cols)]
        return pltpu.make_async_remote_copy(
            src_ref=ref,
            dst_ref=ref,
            send_sem=send_sem.at[i],
            recv_sem=recv_sem.at[i],
            device_id=(target, y),
            device_id_type=MESH,
        )

    def send(slot, rows, cols, target):
        i = count[0]
        count[0] += 1
        copy = copy_of(i, slot, rows, cols, target)
        copy.start()
        started.append(copy)
        return i

    def arrive(i, slot, rows, cols):
        copy_of(i, slot, rows, cols, partner).wait_recv()

    def both_cores(half, dp, dq):
        p, q = pos[half]
        zz, xx = (q + dq, p + dp) if half == 0 else (p + dp, q + dq)
        zz, xx = lax.rem(zz + 4, 4), lax.rem(xx + 4, 4)
        return seq_of(zz, xx, c), seq_of(zz, xx, 1 - c)

    def mine(half, dp, dq):
        return both_cores(half, dp, dq)[0]

    def die(slots, rows):
        slot, theirs = slots
        died.append((send(slot, rows, whole, partner), theirs, rows))

    first, second, across, further = {}, {}, {}, {}

    def spread(half, dp):
        rows = half_rows[half]
        for d in (1, -1):
            second[half, dp, d] = send(mine(half, dp, 0), rows, whole, mine(half, 0, d))
        die(both_cores(half, dp, 0), rows)

    def pass_on(half, dp):
        rows = half_rows[half]
        for d, cols in ways:
            slot = mine(half, dp, -d)
            arrive(second[half, dp, d], slot, rows, whole)
            further[half, dp, d] = send(slot, rows, cols, mine(half, 0, d))
            die(both_cores(half, dp, -d), rows)

    def ended(half, dp):
        rows = half_rows[half]
        for d, cols in ways:
            arrive(further[half, dp, d], mine(half, dp, -2 * d), rows, cols)
        die(both_cores(half, dp, 2), rows)

    for half in (0, 1):
        for d in (1, -1):
            first[half, d] = send(me, half_rows[half], whole, mine(half, d, 0))
    for half in (0, 1):
        for d in (1, -1):
            second[half, 0, d] = send(me, half_rows[half], whole, mine(half, 0, d))
    died.append((send(me, (0, ROWS), whole, partner), partner, (0, ROWS)))
    yield
    for d, cols in ways:
        for half in (0, 1):
            rows = half_rows[half]
            arrive(first[half, d], mine(half, -d, 0), rows, whole)
            across[half, d] = send(mine(half, -d, 0), rows, cols, mine(half, d, 0))
    for d in (1, -1):
        for half in (0, 1):
            spread(half, -d)
    yield
    for half in (0, 1):
        pass_on(half, 0)
    yield
    for half in (0, 1):
        for d, cols in ways:
            arrive(across[half, d], mine(half, -2 * d, 0), half_rows[half], cols)
        spread(half, 2)
    yield
    for dp in (-1, 1):
        for half in (0, 1):
            pass_on(half, dp)
    for half in (0, 1):
        ended(half, 0)
    yield
    for half in (0, 1):
        pass_on(half, 2)
    for dp in (-1, 1, 2):
        for half in (0, 1):
            ended(half, dp)
    for i, slot, rows in died:
        arrive(i, slot, rows, whole)
    yield
    for copy in started:
        copy.wait_send()
    assert count[0] == GATHER_OPS


def own_rows_in(refs, buf, sems):
    me = lax.axis_index("seq")
    copies = []
    at = 0
    for i, ref in enumerate(refs):
        width = ref.shape[1]
        copies.append(
            pltpu.make_async_copy(ref, buf.at[me, :, pl.ds(at, width)], sems.at[i])
        )
        at += width
    return copies


def doc_lanes(docs_ref):
    lane = lax.broadcasted_iota(jnp.int32, (1, 128), 1)
    first = jnp.where((lane >= ONES) & (lane < FLAG), -1, FAR)
    last = jnp.full((1, 128), FAR, jnp.int32)
    bound = jnp.int32(0)
    for k in range(NDOCS):
        first = jnp.where(lane == k, bound, first)
        bound = bound + docs_ref[k]
        last = jnp.where(lane == k, bound, last)
    return lane, first, last


def first_start(docs_ref, place_):
    bound = jnp.int32(0)
    lo = jnp.int32(0)
    for k in range(NDOCS):
        bound = bound + docs_ref[k]
        lo = jnp.where(bound <= place_, bound, lo)
    return lo


def key_marks(at, count, limit, lanes):
    lane, first, last = lanes
    first = jnp.where(lane == FLAG, limit, first)
    places = at + lax.broadcasted_iota(jnp.int32, (count, 128), 0)
    inside = (places >= first) & (places < last)
    return inside.astype(jnp.float32).astype(jnp.bfloat16)


def stack_heads(dst, src, first_head, ratio):
    for h in range(ratio):
        cols = slice((first_head + h) * HD, (first_head + h + 1) * HD)
        dst[h * 128 : (h + 1) * 128, 0:HD] = src[0:128, cols]
        dst[ratio * 128 + h * 32 : ratio * 128 + (h + 1) * 32, 0:HD] = src[128:160, cols]


def parts(value):
    high = value.astype(jnp.bfloat16).astype(jnp.float32)
    rest = value - high
    middle = rest.astype(jnp.bfloat16).astype(jnp.float32)
    return high, middle, rest - middle


def query_marks(places, shift, lanes):
    lane, first, last = lanes
    inside = (places >= first) & (places < last)
    marks = jnp.where((lane < NDOCS) & jnp.logical_not(inside) | (lane == FLAG), LOW, 0.0)
    for k, part in enumerate(parts(-shift)):
        marks = jnp.where(lane == ONES + k, part, marks)
    return marks.astype(jnp.bfloat16)


def mark_queries(dst, keys, place_, lanes, ratio):
    for begin, count, base in ((0, 128, 0), (128, 32, ratio * 128)):
        own = keys[begin : begin + count, :].astype(jnp.float32)
        places = place_ + begin + lax.broadcasted_iota(jnp.int32, (count, 1), 0)
        for h in range(ratio):
            rows = slice(base + h * count, base + (h + 1) * count)
            q = dst[rows, 0:HD].astype(jnp.float32)
            shift = jnp.sum(q * own, axis=1, keepdims=True)
            dst[rows, HD:] = query_marks(places, shift, lanes)


def lane_rows(ratio):
    lane = lax.broadcasted_iota(jnp.int32, (1, ratio * ROWS), 1)
    cut = ratio * 128
    return jnp.where(lane < cut, lane & 127, 128 + ((lane - cut) & 31))


def chunks(width):
    return [(a, min(a + CHUNK, width)) for a in range(0, width, CHUNK)]


def own_pairs(a, b, lanes_row):
    return lax.broadcasted_iota(jnp.int32, (ROWS, b - a), 0) <= lanes_row[:, a:b]


class Window:
    def __init__(self, docs_ref, gath, first_col, own, blocks, own_sem, sems, size):
        self.place = lax.axis_index("seq") * ROWS
        self.lo = first_start(docs_ref, self.place)
        self.size = size
        self.gath, self.own, self.blocks = gath, own, blocks
        self.own_sem, self.sems = own_sem, sems
        self.cols = pl.ds(first_col, own.shape[1])
        self.steps = (jnp.maximum(self.place - self.lo, 0) + size - 1) // size
        self.lanes = doc_lanes(docs_ref)

    def at(self, step):
        return pl.multiple_of(jnp.maximum(self.place - (step + 1) * self.size, 0), 16)

    def own_copy(self):
        rows = pl.ds(pl.multiple_of(self.place, 16), ROWS)
        return pltpu.make_async_copy(self.gath.at[rows, self.cols], self.own, self.own_sem)

    def copy(self, step):
        rows = pl.ds(self.at(step), self.size)
        return pltpu.make_async_copy(
            self.gath.at[rows, self.cols], self.blocks.at[step], self.sems.at[step]
        )

    def start(self):
        self.own_copy().start()
        self.start_blocks()

    def start_blocks(self):
        @pl.loop(0, self.steps)
        def _(step):
            self.copy(step).start()

    def wait_blocks(self):
        @pl.loop(0, self.steps)
        def _(step):
            self.copy(step).wait()

    def marks(self, step):
        return key_marks(
            self.at(step), self.size, self.place - step * self.size, self.lanes
        )

    def own_marks(self):
        return key_marks(self.place, ROWS, jnp.int32(FAR), self.lanes)


def extended(values):
    ones = jnp.ones((16, values.shape[0]), jnp.bfloat16)
    return jnp.concatenate([jnp.transpose(values), ones], axis=0)


class Attention:
    def __init__(self, queries, sums, acc, top, ratio):
        self.queries, self.sums, self.acc, self.top = queries, sums, acc, top
        self.lanes_row = lane_rows(ratio)
        self.chunks = chunks(ratio * ROWS)

    def pieces(self, kv, marks, own):
        groups = len(self.queries)
        for g in range(groups):
            keys = jnp.concatenate([kv[:, g * HD : (g + 1) * HD], marks], axis=1)
            values = extended(kv[:, (groups + g) * HD : (groups + g + 1) * HD])
            for a, b in self.chunks:
                s = dot(keys, self.queries[g][a:b, :], NT)
                if own:
                    s = jnp.where(own_pairs(a, b, self.lanes_row), s, MASKED)
                yield g, a, b, s, values

    def sum_rows(self, p):
        return jnp.sum(p.reshape(p.shape[0] // 8, 8, p.shape[1]), axis=0)

    def block(self, kv, marks, own):
        sums, acc = self.sums, self.acc
        if own:
            self.top[...] = jnp.zeros(self.top.shape, jnp.float32)
        for g, a, b, s, values in self.pieces(kv, marks, own):
            p = jnp.exp2(s * EXP2_SCALE)
            add = dot(values, p.astype(jnp.bfloat16))
            if sums is not None:
                total = self.sum_rows(p)
                sums[g, :, a:b] = total if own else sums[g, :, a:b] + total
            acc[g, :, a:b] = add if own else acc[g, :, a:b] + add

    def safe_block(self, kv, marks, own):
        sums, acc, top = self.sums, self.acc, self.top
        for g, a, b, s, values in self.pieces(kv, marks, own):
            old = jnp.full((1, b - a), LOW) if own else top[g, :, a:b]
            new = jnp.maximum(old, jnp.max(s, axis=0, keepdims=True))
            p = jnp.exp2((s - new) * EXP2_SCALE)
            add = dot(values, p.astype(jnp.bfloat16))
            top[g, :, a:b] = new
            alpha = None if own else jnp.exp2((old - new) * EXP2_SCALE)
            if sums is not None:
                total = self.sum_rows(p)
                sums[g, :, a:b] = total if own else sums[g, :, a:b] * alpha + total
            acc[g, :, a:b] = add if own else acc[g, :, a:b] * alpha + add

    def safe_window(self, window):
        self.safe_block(window.own, window.own_marks(), True)

        @pl.loop(0, window.steps)
        def _(step):
            self.safe_block(window.blocks.at[step], window.marks(step), False)


def too_large(weight_sums):
    return jnp.logical_not(jnp.max(weight_sums) < 2.0**100)


def member_rows(spans_ref):
    start = spans_ref[0, 0:1, :]
    length = spans_ref[0, 1:2, :]
    row = lax.broadcasted_iota(jnp.int32, (ROWS, SLOTS), 0)
    inside = (row >= start) & (row < start + length)
    weight = 1.0 / jnp.maximum(length, 1).astype(jnp.float32)
    return inside.astype(jnp.float32), weight, length


def forward_kernel(
    tdocs, tq, gath, tspans, pooled, stack, own, blocks, acc, top, own_sem, sem
):
    window = Window(tdocs, gath, 0, own, blocks, own_sem, sem, FB)
    window.start()
    for g in range(TG):
        stack_heads(stack.at[g], tq, g * TR, TR)
    window.own_copy().wait()
    for g in range(TG):
        mark_queries(
            stack.at[g], own.at[:, g * HD : (g + 1) * HD], window.place, window.lanes, TR
        )
    attention = Attention([stack.at[g] for g in range(TG)], None, acc, top, TR)
    attention.block(own, window.own_marks(), True)

    @pl.loop(0, window.steps)
    def _(step):
        window.copy(step).wait()
        attention.block(blocks.at[step], window.marks(step), False)

    @pl.when(too_large(acc[:, HD : HD + 8, :]))
    def _():
        attention.safe_window(window)

    member, weight, _ = member_rows(tspans)
    member = member.astype(jnp.bfloat16)
    tail = jnp.concatenate([member[128:160]] * TR, axis=0)
    owner = lax.broadcasted_iota(jnp.int32, (TR * 32, SLOTS), 0) // 32
    for g in range(TG):
        inverse = 1.0 / acc[g, HD : HD + 1]
        context_t = (acc[g, 0:HD] * inverse).astype(jnp.bfloat16)
        for h in range(TR):
            sums = dot(context_t[:, h * 128 : (h + 1) * 128], member[0:128]) + dot(
                context_t[:, TR * 128 :], jnp.where(owner == h, tail, jnp.zeros_like(tail))
            )
            cols = slice((g * TR + h) * HD, (g * TR + h + 1) * HD)
            pooled[:, cols] = jnp.transpose(sums * weight).astype(jnp.bfloat16)


def forward(tdocs, tq, gath, tspans):
    vmem = pl.BlockSpec(memory_space=pltpu.VMEM)
    smem = pl.BlockSpec(memory_space=pltpu.SMEM)
    hbm = pl.BlockSpec(memory_space=pl.ANY)
    tw = TR * ROWS
    bf16, f32 = jnp.bfloat16, jnp.float32
    return pl.pallas_call(
        forward_kernel,
        out_shape=jax.ShapeDtypeStruct((SLOTS, TG * TR * HD), bf16),
        in_specs=[smem, vmem, hbm, vmem],
        out_specs=vmem,
        scratch_shapes=[
            pltpu.VMEM((TG, tw, 2 * HD), bf16),
            pltpu.VMEM((ROWS, 2 * TG * HD), bf16),
            pltpu.VMEM((STEPS, FB, 2 * TG * HD), bf16),
            pltpu.VMEM((TG, HD + 16, tw), f32),
            pltpu.VMEM((TG, 1, tw), f32),
            pltpu.SemaphoreType.DMA,
            pltpu.SemaphoreType.DMA((STEPS,)),
        ],
        compiler_params=pltpu.CompilerParams(vmem_limit_bytes=34 * MIB),
        name="forward",
    )(tdocs, tq, gath, tspans)


def student_results(attention, stack, lanes, sctx, qback):
    acc = attention.acc
    total = jnp.sum(attention.sums[0], axis=0, keepdims=True)
    inverse = 1.0 / acc[0, HD : HD + 1]
    extra = attention.top[0] + jnp.log2(total) * (1.0 / EXP2_SCALE)
    for h in range(SR):
        cols = slice(h * 128, (h + 1) * 128)
        sctx[0:128, cols] = jnp.transpose(acc[0, 0:HD, cols] * inverse[:, cols]).astype(
            jnp.bfloat16
        )
    rest = jnp.transpose(acc[0, 0:HD, SR * 128 :] * inverse[:, SR * 128 :]).astype(jnp.bfloat16)
    for h in range(SR):
        sctx[128:160, h * HD : (h + 1) * HD] = rest[h * 32 : (h + 1) * 32]
    qback[:, 0:HD] = stack[:, 0:HD]
    lane = lanes[0]
    ones = (lane >= ONES) & (lane < FLAG)
    for a in range(0, SR * ROWS, 128):
        b = min(a + 128, SR * ROWS)
        column = jnp.transpose(jnp.broadcast_to(extra[:, a:b], (8, b - a)))[:, 0:1]
        marks = stack[a:b, HD:].astype(jnp.float32)
        before = jnp.sum(jnp.where(ones, marks, 0.0), axis=1, keepdims=True)
        for k, part in enumerate(parts(before - column)):
            marks = jnp.where(lane == ONES + k, part, marks)
        qback[a:b, HD:] = marks.astype(jnp.bfloat16)


def gather_kernel(tk, tv, sk, sv, gath, own_sem, send_sem, recv_sem):
    y = lax.axis_index("mp")
    copies = own_rows_in((tk, tv, sk, sv), gath, own_sem)
    for copy in copies:
        copy.start()
    greet([(peer, y) for peer in seq_neighbours()])
    for copy in copies:
        copy.wait()
    for _ in torus_gather(gath, send_sem, recv_sem):
        pass


def gather(tk, tv, sk, sv):
    hbm = pl.BlockSpec(memory_space=pl.ANY)
    return pl.pallas_call(
        gather_kernel,
        out_shape=jax.ShapeDtypeStruct((SEQ, ROWS, TKV + SKV), jnp.bfloat16),
        in_specs=[hbm] * 4,
        out_specs=pl.BlockSpec(memory_space=pltpu.VMEM),
        scratch_shapes=[
            pltpu.SemaphoreType.DMA((4,)),
            pltpu.SemaphoreType.DMA((GATHER_OPS,)),
            pltpu.SemaphoreType.DMA((GATHER_OPS,)),
        ],
        compiler_params=pltpu.CompilerParams(
            collective_id=0, has_side_effects=True, vmem_limit_bytes=12 * MIB
        ),
        name="gather",
    )(tk, tv, sk, sv)


def align_kernel(
    sdocs, pooled, projector, gath, sk, sv, sq, arrived, sctx, qback, weight_sums,
    wide, part, near, far, blocks, landed, kv, stack, sums, acc, top,
    load_sem, send_sem, recv_sem, a2a_send, a2a_recv, own_sem,
):
    me = lax.axis_index("seq")
    y = lax.axis_index("mp")
    cols = part.shape[2]
    half = SLOTS // 2
    up, down, across = lax.rem(y + 1, 4), lax.rem(y + 3, 4), lax.rem(y + 2, 4)
    order = (across, up, down, y)
    loads = []
    for i, target in enumerate(order):
        begin = pl.multiple_of(target * cols, 128)
        copy = pltpu.make_async_copy(
            projector.at[:, pl.ds(begin, cols)], wide.at[i], load_sem.at[i]
        )
        copy.start()
        loads.append(copy)
    student = pltpu.make_async_copy(gath.at[:, pl.ds(TKV, SKV)], kv, own_sem.at[1])
    student.start()

    barrier = pltpu.get_barrier_semaphore()
    for target in (up, down):
        pl.semaphore_signal(barrier, inc=1, device_id=(me, target), device_id_type=MESH)

    @pl.loop(1, SEQ)
    def _(k):
        pl.semaphore_signal(
            barrier, inc=1, device_id=(lax.rem(me + k, SEQ), y), device_id_type=MESH
        )

    pl.semaphore_wait(barrier, SEQ + 1)

    def project(i):
        loads[i].wait()
        return dot(pooled[...], wide[i])

    def remote(i, src, dst, target):
        return pltpu.make_async_remote_copy(
            src_ref=src,
            dst_ref=dst,
            send_sem=send_sem.at[i],
            recv_sem=recv_sem.at[i],
            device_id=(me, target),
            device_id_type=MESH,
        )

    low, high = pl.ds(0, half), pl.ds(half, half)
    hops = [
        remote(0, part.at[0, low], far.at[0], up),
        remote(1, part.at[0, high], far.at[1], down),
        remote(2, part.at[1, high], near.at[0, high], up),
        remote(3, part.at[2, low], near.at[1, low], down),
        remote(4, part.at[1, low], near.at[0, low], up),
        remote(5, part.at[2, high], near.at[1, high], down),
    ]
    part[0] = project(0).astype(jnp.bfloat16)
    hops[0].start()
    hops[1].start()
    for_up = project(1)
    part[1, half:] = for_up[half:].astype(jnp.bfloat16)
    hops[2].start()
    for_down = project(2)
    part[2, :half] = for_down[:half].astype(jnp.bfloat16)
    hops[3].start()
    place_ = me * ROWS
    lanes = doc_lanes(sdocs)
    stack_heads(stack, sq, 0, SR)
    mark_queries(stack, sk[...], place_, lanes, SR)
    attention = Attention([stack], sums, acc, top, SR)
    attention.block(
        jnp.concatenate([sk[...], sv[...]], axis=1),
        key_marks(place_, ROWS, jnp.int32(FAR), lanes),
        True,
    )
    count = (place_ + SB - 1) // SB

    def student_blocks(first, last):
        @pl.loop(first, last)
        def _(b):
            rows = pl.ds(pl.multiple_of(b * SB, SB), SB)
            attention.block(kv[rows], key_marks(b * SB, SB, place_, lanes), False)

    student.wait()
    hops[0].wait_recv()
    part[1, :half] = (for_up[:half] + far[0].astype(jnp.float32)).astype(jnp.bfloat16)
    hops[4].start()
    hops[1].wait_recv()
    part[2, half:] = (for_down[half:] + far[1].astype(jnp.float32)).astype(jnp.bfloat16)
    hops[5].start()
    mine = project(3)
    student_blocks(0, count // 2)
    for i in (2, 3, 4, 5):
        hops[i].wait_recv()
    total = mine + near[0].astype(jnp.float32) + near[1].astype(jnp.float32)
    for d in range(SEQ):
        blocks[d] = total[4 * d : 4 * d + 4].astype(jnp.bfloat16)

    def exchange(k, src, target):
        return pltpu.make_async_remote_copy(
            src_ref=blocks.at[target],
            dst_ref=landed.at[src],
            send_sem=a2a_send.at[k],
            recv_sem=a2a_recv.at[k],
            device_id=(target, y),
            device_id_type=MESH,
        )

    @pl.loop(1, SEQ)
    def _(k):
        exchange(k, me, lax.rem(me + k, SEQ)).start()

    own = pltpu.make_async_copy(blocks.at[me], landed.at[me], own_sem.at[0])
    own.start()
    student_blocks(count // 2, count)
    weight_sums[...] = acc[0, HD : HD + 8, :]
    student_results(attention, stack, lanes, sctx, qback)
    own.wait()

    @pl.loop(1, SEQ)
    def _(k):
        exchange(k, lax.rem(me + SEQ - k, SEQ), lax.rem(me + k, SEQ)).wait_recv()

    for s in range(SEQ):
        arrived[4 * s : 4 * s + 4, :] = landed[s].astype(jnp.float32)

    @pl.loop(1, SEQ)
    def _(k):
        exchange(k, me, lax.rem(me + k, SEQ)).wait_send()

    for hop in hops:
        hop.wait_send()


def align(sdocs, pooled, projector, gath, sk, sv, sq):
    vmem = pl.BlockSpec(memory_space=pltpu.VMEM)
    smem = pl.BlockSpec(memory_space=pltpu.SMEM)
    hbm = pl.BlockSpec(memory_space=pl.ANY)
    depth, width = projector.shape
    cols = width // 4
    sw = SR * ROWS
    bf16, f32 = jnp.bfloat16, jnp.float32
    return pl.pallas_call(
        align_kernel,
        out_shape=(
            jax.ShapeDtypeStruct((SLOTS, cols), f32),
            jax.ShapeDtypeStruct((ROWS, SR * HD), bf16),
            jax.ShapeDtypeStruct((sw, 2 * HD), bf16),
            jax.ShapeDtypeStruct((8, sw), f32),
        ),
        in_specs=[smem, vmem, hbm, hbm, vmem, vmem, vmem],
        out_specs=(vmem,) * 4,
        scratch_shapes=[
            pltpu.VMEM((4, depth, cols), bf16),
            pltpu.VMEM((3, SLOTS, cols), bf16),
            pltpu.VMEM((2, SLOTS, cols), bf16),
            pltpu.VMEM((2, SLOTS // 2, cols), bf16),
            pltpu.VMEM((SEQ, 4, cols), bf16),
            pltpu.VMEM((SEQ, 4, cols), bf16),
            pltpu.VMEM((TOKENS, SKV), bf16),
            pltpu.VMEM((sw, 2 * HD), bf16),
            pltpu.VMEM((1, 8, sw), f32),
            pltpu.VMEM((1, HD + 16, sw), f32),
            pltpu.VMEM((1, 1, sw), f32),
            pltpu.SemaphoreType.DMA((4,)),
            pltpu.SemaphoreType.DMA((6,)),
            pltpu.SemaphoreType.DMA((6,)),
            pltpu.SemaphoreType.DMA((SEQ,)),
            pltpu.SemaphoreType.DMA((SEQ,)),
            pltpu.SemaphoreType.DMA((2,)),
        ],
        compiler_params=pltpu.CompilerParams(
            collective_id=1, has_side_effects=True, vmem_limit_bytes=38 * MIB
        ),
        name="align",
    )(sdocs, pooled, projector, gath, sk, sv, sq)


def backward_kernel(
    sdocs, qback_in, gath, sctx_in, weight_sums, sq, arrived, sspans, grad_q, terms,
    dstack, dq_t, own, blocks, qback, sctx, stack, sums, acc, top, own_sem, sem,
):
    window = Window(sdocs, gath, TKV, own, blocks, own_sem, sem, BB)
    window.start()
    qback[...] = qback_in[...]
    sctx[...] = sctx_in[...]
    window.own_copy().wait()

    @pl.when(too_large(weight_sums[...]))
    def _():
        window.wait_blocks()
        stack_heads(stack, sq, 0, SR)
        mark_queries(stack, own.at[:, 0:HD], window.place, window.lanes, SR)
        attention = Attention([stack], sums, acc, top, SR)
        attention.safe_window(window)
        student_results(attention, stack, window.lanes, sctx, qback)
        window.start_blocks()

    width = SR * ROWS
    terms[...] = jnp.zeros(terms.shape, terms.dtype)
    member, weight, length = member_rows(sspans)
    columns = jnp.transpose(
        jnp.concatenate(
            [weight, (length > 0).astype(jnp.float32), jnp.zeros((6, SLOTS), jnp.float32)],
            axis=0,
        )
    )
    weight, live = columns[:, 0:1], columns[:, 1:2]
    member_t = jnp.transpose(member).astype(jnp.bfloat16)
    member = member.astype(jnp.bfloat16)
    pooled = dot(member_t, sctx[...]) * weight
    gap = jnp.where(live > 0.0, pooled - arrived[...], 0.0) * weight
    high = gap.astype(jnp.bfloat16)
    low = (gap - high.astype(jnp.float32)).astype(jnp.bfloat16)
    dout = (dot(member, high) + dot(member, low)).astype(jnp.bfloat16)
    lane = window.lanes[0]
    for h in range(SR):
        cols = slice(h * HD, (h + 1) * HD)
        head = dout[:, cols]
        delta = jnp.sum(
            head.astype(jnp.float32) * sctx[:, cols].astype(jnp.float32), axis=1, keepdims=True
        )
        marks = jnp.zeros((ROWS, 128), jnp.float32)
        for k, part in enumerate(parts(-delta)):
            marks = jnp.where(lane == ONES + k, part, marks)
        marks = marks.astype(jnp.bfloat16)
        top = slice(h * 128, (h + 1) * 128)
        rest = slice(SR * 128 + h * 32, SR * 128 + (h + 1) * 32)
        dstack[top, 0:HD] = head[0:128]
        dstack[rest, 0:HD] = head[128:160]
        dstack[top, HD:] = marks[0:128]
        dstack[rest, HD:] = marks[128:160]

    lanes_row = lane_rows(SR)

    def block(kv, marks, at, own_rows):
        count = kv.shape[0]
        rows = pl.ds(at, count)
        plain = kv[:, 0:HD]
        keys = jnp.concatenate([plain, marks], axis=1)
        values = jnp.concatenate([kv[:, HD:], marks], axis=1)
        keys_t = jnp.transpose(plain)
        grad_k = jnp.zeros((count, HD), jnp.float32)
        grad_v = jnp.zeros((count, HD), jnp.float32)
        for a, b in chunks(width):
            p = jnp.exp2(dot(keys, qback[a:b, :], NT) * EXP2_SCALE)
            if own_rows:
                p = jnp.where(own_pairs(a, b, lanes_row), p, 0.0)
            ds = (p * dot(values, dstack[a:b, :], NT)).astype(jnp.bfloat16)
            grad_v = grad_v + dot(p.astype(jnp.bfloat16), dstack[a:b, 0:HD])
            grad_k = grad_k + dot(ds, qback[a:b, 0:HD])
            add = dot(keys_t, ds)
            if own_rows:
                dq_t[:, a:b] = add
            else:
                dq_t[:, a:b] += add
        grad = jnp.concatenate([grad_k * SCALE, grad_v], axis=1)
        if not own_rows:
            grad = grad + terms[rows, :].astype(jnp.float32)
        terms[rows, :] = grad.astype(jnp.bfloat16)

    block(window.own, window.own_marks(), pl.multiple_of(window.place, 16), True)

    @pl.loop(0, window.steps)
    def _(step):
        window.copy(step).wait()
        block(window.blocks.at[step], window.marks(step), window.at(step), False)

    for h in range(SR):
        cols = slice(h * HD, (h + 1) * HD)
        grad_q[0:128, cols] = (jnp.transpose(dq_t[:, h * 128 : (h + 1) * 128]) * SCALE).astype(
            jnp.bfloat16
        )
    rest = (jnp.transpose(dq_t[:, SR * 128 :]) * SCALE).astype(jnp.bfloat16)
    for h in range(SR):
        grad_q[128:160, h * HD : (h + 1) * HD] = rest[h * 32 : (h + 1) * 32]


def backward(sdocs, qback, gath, sctx, weight_sums, sq, arrived, sspans):
    vmem = pl.BlockSpec(memory_space=pltpu.VMEM)
    smem = pl.BlockSpec(memory_space=pltpu.SMEM)
    hbm = pl.BlockSpec(memory_space=pl.ANY)
    sw = SR * ROWS
    bf16 = jnp.bfloat16
    return pl.pallas_call(
        backward_kernel,
        out_shape=(
            jax.ShapeDtypeStruct((ROWS, SR * HD), bf16),
            jax.ShapeDtypeStruct((TOKENS, 2 * HD), bf16),
        ),
        in_specs=[smem, vmem, hbm, vmem, vmem, vmem, vmem, vmem],
        out_specs=(vmem, vmem),
        scratch_shapes=[
            pltpu.VMEM((sw, 2 * HD), bf16),
            pltpu.VMEM((HD, sw), jnp.float32),
            pltpu.VMEM((ROWS, 2 * HD), bf16),
            pltpu.VMEM((STEPS, BB, 2 * HD), bf16),
            pltpu.VMEM((sw, 2 * HD), bf16),
            pltpu.VMEM((ROWS, SR * HD), bf16),
            pltpu.VMEM((sw, 2 * HD), bf16),
            pltpu.VMEM((1, 8, sw), jnp.float32),
            pltpu.VMEM((1, HD + 16, sw), jnp.float32),
            pltpu.VMEM((1, 1, sw), jnp.float32),
            pltpu.SemaphoreType.DMA,
            pltpu.SemaphoreType.DMA((STEPS,)),
        ],
        compiler_params=pltpu.CompilerParams(vmem_limit_bytes=34 * MIB),
        name="backward",
    )(sdocs, qback, gath, sctx, weight_sums, sq, arrived, sspans)


def scatter_kernel(
    terms, pieces, theirs, ours, chip, far1, near1, out1, far2,
    die_send, die_recv, own_sem, send_sem, recv_sem,
):
    me, z, x, c = place()
    y = lax.axis_index("mp")
    partner = seq_of(z, x, 1 - c)
    wrap = lambda v: lax.rem(v + 4, 4)

    def peer(axis, d):
        return seq_of(wrap(z + d), x, c) if axis == "z" else seq_of(z, wrap(x + d), c)

    f32 = lambda v: v.astype(jnp.float32)
    axes = (("z", "x"), ("x", "z"))
    pos = ((z, x), (x, z))

    def terms_of(h, i, core):
        rows = pl.ds(80 * h, 80)
        return terms.at[i, :, core, rows] if h == 0 else terms.at[:, i, core, rows]

    order = (2, 1, 3, 0)

    def own_copy(h, k):
        i = wrap(pos[h][0] + order[k])
        return pltpu.make_async_copy(
            terms_of(h, i, c), ours.at[h, i], own_sem.at[4 * h + k]
        )

    for k in range(4):
        for h in (0, 1):
            own_copy(h, k).start()

    greet(
        [(peer("z", 1), y), (peer("z", 3), y), (peer("x", 1), y), (peer("x", 3), y)]
        + [(partner, y)]
    )

    def crossing(h, k):
        i = wrap(pos[h][0] + order[k])
        return pltpu.make_async_remote_copy(
            src_ref=terms_of(h, i, 1 - c),
            dst_ref=theirs.at[h, i],
            send_sem=die_send.at[4 * h + k],
            recv_sem=die_recv.at[4 * h + k],
            device_id=(partner, y),
            device_id_type=MESH,
        )

    def both_cores(h, k):
        i = wrap(pos[h][0] + order[k])
        own_copy(h, k).wait()
        crossing(h, k).wait_recv()
        chip[h, i] = (f32(ours[h, i]) + f32(theirs[h, i])).astype(jnp.bfloat16)

    for k in range(4):
        for h in (0, 1):
            crossing(h, k).start()

    def remote(i, src, dst, target):
        return pltpu.make_async_remote_copy(
            src_ref=src,
            dst_ref=dst,
            send_sem=send_sem.at[i],
            recv_sem=recv_sem.at[i],
            device_id=(target, y),
            device_id_type=MESH,
        )

    all_hops = []
    first = []
    for h in (0, 1):
        axis = axes[h][0]
        p = pos[h][0]
        up, down = peer(axis, 1), peer(axis, 3)
        to_far, to_up, to_down = wrap(p + 2), wrap(p + 1), wrap(p + 3)
        lo, hi = pl.ds(0, 2), pl.ds(2, 2)
        hops = [
            remote(12 * h + 0, chip.at[h, to_far, lo], far1.at[h, 0], up),
            remote(12 * h + 1, chip.at[h, to_far, hi], far1.at[h, 1], down),
            remote(12 * h + 2, chip.at[h, to_up, hi], near1.at[h, 0, hi], up),
            remote(12 * h + 3, chip.at[h, to_down, lo], near1.at[h, 1, lo], down),
            remote(12 * h + 4, chip.at[h, to_up, lo], near1.at[h, 0, lo], up),
            remote(12 * h + 5, chip.at[h, to_down, hi], near1.at[h, 1, hi], down),
        ]
        first.append((hops, to_up, to_down))
        all_hops += hops
    for k, ready in enumerate(((0, 1), (2,), (3,), ())):
        for h in (0, 1):
            both_cores(h, k)
            for i in ready:
                first[h][0][i].start()
    for h in (0, 1):
        hops, to_up, to_down = first[h]
        lo, hi = pl.ds(0, 2), pl.ds(2, 2)
        hops[0].wait_recv()
        chip[h, to_up, lo] = (f32(chip[h, to_up, lo]) + f32(far1[h, 0])).astype(jnp.bfloat16)
        hops[4].start()
        hops[1].wait_recv()
        chip[h, to_down, hi] = (f32(chip[h, to_down, hi]) + f32(far1[h, 1])).astype(jnp.bfloat16)
        hops[5].start()
    second = []
    for h in (0, 1):
        hops = first[h][0]
        for k in range(2, 6):
            hops[k].wait_recv()
        out1[h] = (f32(chip[h, pos[h][0]]) + f32(near1[h, 0]) + f32(near1[h, 1])).astype(
            jnp.bfloat16
        )
        axis = axes[h][1]
        p = pos[h][1]
        up, down = peer(axis, 1), peer(axis, 3)
        to_far, to_up, to_down = wrap(p + 2), wrap(p + 1), wrap(p + 3)
        lo, hi = pl.ds(0, HD), pl.ds(HD, HD)
        rows = pl.ds(0, 80)
        hops = [
            remote(12 * h + 6, out1.at[h, to_far, rows, lo], far2.at[h, 0], up),
            remote(12 * h + 7, out1.at[h, to_far, rows, hi], far2.at[h, 1], down),
            remote(12 * h + 8, out1.at[h, to_up, rows, hi], pieces.at[h, 1, rows, hi], up),
            remote(12 * h + 9, out1.at[h, to_down, rows, lo], pieces.at[h, 2, rows, lo], down),
            remote(12 * h + 10, out1.at[h, to_up, rows, lo], pieces.at[h, 1, rows, lo], up),
            remote(12 * h + 11, out1.at[h, to_down, rows, hi], pieces.at[h, 2, rows, hi], down),
        ]
        for k in range(4):
            hops[k].start()
        second.append((hops, to_up, to_down))
        all_hops += hops
    for h in (0, 1):
        hops, to_up, to_down = second[h]
        hops[0].wait_recv()
        out1[h, to_up, :, 0:HD] = (f32(out1[h, to_up, :, 0:HD]) + f32(far2[h, 0])).astype(
            jnp.bfloat16
        )
        hops[4].start()
        hops[1].wait_recv()
        out1[h, to_down, :, HD:] = (f32(out1[h, to_down, :, HD:]) + f32(far2[h, 1])).astype(
            jnp.bfloat16
        )
        hops[5].start()
    for h in (0, 1):
        hops = second[h][0]
        for k in range(2, 6):
            hops[k].wait_recv()
        pieces[h, 0] = out1[h, pos[h][1]]
    for hop in all_hops:
        hop.wait_send()
    for h in (0, 1):
        for k in range(4):
            crossing(h, k).wait_send()


def scatter(terms):
    vmem = pl.BlockSpec(memory_space=pltpu.VMEM)
    bf16 = jnp.bfloat16
    width = terms.shape[-1]
    return pl.pallas_call(
        scatter_kernel,
        out_shape=jax.ShapeDtypeStruct((2, 3, 80, width), bf16),
        in_specs=[pl.BlockSpec(memory_space=pl.ANY)],
        out_specs=vmem,
        scratch_shapes=[
            pltpu.VMEM((2, 4, 4, 80, width), bf16),
            pltpu.VMEM((2, 4, 4, 80, width), bf16),
            pltpu.VMEM((2, 4, 4, 80, width), bf16),
            pltpu.VMEM((2, 2, 2, 80, width), bf16),
            pltpu.VMEM((2, 2, 4, 80, width), bf16),
            pltpu.VMEM((2, 4, 80, width), bf16),
            pltpu.VMEM((2, 2, 80, HD), bf16),
            pltpu.SemaphoreType.DMA((8,)),
            pltpu.SemaphoreType.DMA((8,)),
            pltpu.SemaphoreType.DMA((8,)),
            pltpu.SemaphoreType.DMA((24,)),
            pltpu.SemaphoreType.DMA((24,)),
        ],
        compiler_params=pltpu.CompilerParams(
            collective_id=2, has_side_effects=True, vmem_limit_bytes=18 * MIB
        ),
        name="scatter",
    )(terms)


def total_kernel(pieces, grad_k, grad_v):
    for h in (0, 1):
        rows = slice(80 * h, 80 * h + 80)
        total = sum(pieces[h, k].astype(jnp.float32) for k in range(3)).astype(jnp.bfloat16)
        grad_k[rows, :] = total[:, 0:HD]
        grad_v[rows, :] = total[:, HD:]


def total(pieces):
    vmem = pl.BlockSpec(memory_space=pltpu.VMEM)
    return pl.pallas_call(
        total_kernel,
        out_shape=(jax.ShapeDtypeStruct((ROWS, HD), jnp.bfloat16),) * 2,
        in_specs=[vmem],
        out_specs=(vmem, vmem),
        compiler_params=pltpu.CompilerParams(vmem_limit_bytes=8 * MIB),
        name="total",
    )(pieces)


def body(
    teacher_query,
    teacher_keys,
    teacher_values,
    teacher_docs,
    student_query,
    student_keys,
    student_values,
    student_docs,
    projector,
    teacher_spans,
    student_spans,
):
    gath = gather(
        *(
            pltpu.with_memory_space_constraint(x, pltpu.HBM)
            for x in (teacher_keys, teacher_values, student_keys, student_values)
        )
    )
    gath = gath.reshape(TOKENS, TKV + SKV)
    pooled = forward(teacher_docs, teacher_query, gath, teacher_spans)
    arrived, sctx, qback, weight_sums = align(
        student_docs, pooled, projector, gath, student_keys, student_values, student_query
    )
    grad_q, terms = backward(
        student_docs, qback, gath, sctx, weight_sums, student_query, arrived, student_spans
    )
    grad_k, grad_v = total(scatter(terms.reshape(4, 4, 2, ROWS, 2 * HD)))
    return grad_q, grad_k, grad_v


def solution(mesh):
    return jax.shard_map(
        body,
        mesh=mesh,
        in_specs=(
            P("seq", "mp"),
            P("seq", "mp"),
            P("seq", "mp"),
            P(),
            P("seq", "mp"),
            P("seq", "mp"),
            P("seq", "mp"),
            P(),
            P("mp", None),
            P("seq", None, None),
            P("seq", None, None),
        ),
        out_specs=(P("seq", "mp"), P("seq", "mp"), P("seq", "mp")),
        check_vma=False,
    )
```
